32 devices in a mesh: replica: 1 (over z), data: 4 (over y), model: 8 (over x, core).
Axes of the slice: x: 4, y: 4, z: 1, core: 2. Of those that a mesh axis runs over, the one named last changes fastest.
The devices are a block of a 4x4x8 slice.
Arguments:
- x_in: bfloat16 [32768, 1024], P(('replica', 'data'))
- w_in: bfloat16 [1024, 1024], P(('replica', 'model'))
- w_mid: bfloat16 [1024, 1024], P(('replica', 'model'))
- w_out: bfloat16 [1024, 1024], P(('replica', 'model'))
- u_in: float32 [1024], P(('replica', 'model'))
- u_mid: float32 [1024], P(('replica', 'model'))
- u_out: float32 [1024], P(('replica', 'model'))
- target: bfloat16 [32768, 1024], P(('replica', 'data'), 'model')
Outputs:
- output 1: float32 [1], P('replica')
- output 2: bfloat16 [32768, 1024], P(('replica', 'data'))
- output 3: float32 [1024, 1024], P(('replica', 'model'))
- output 4: float32 [1024, 1024], P(('replica', 'model'))
- output 5: float32 [1024, 1024], P(('replica', 'model'))
- output 6: float32 [1024], P(('replica', 'model'))
- output 7: float32 [1024], P(('replica', 'model'))
- output 8: float32 [1024], P(('replica', 'model'))
- output 9: float32 [1024], P('replica')
- output 10: float32 [1024], P('replica')
- output 11: float32 [1024], P('replica')
- output 12: float32 [3], P('replica')
All inputs are finite; a program needn't handle non-finite values.
Results may differ from the reference program's by a relative error of at most 0.02.
Values are sent between devices in bfloat16 or wider.
A program may use at most 768 MiB of HBM per device.

```python
import jax
import jax.numpy as jnp

MODEL_DIM = 1024
HIDDEN_DIM = 1024
BATCH_ROWS = 32768


def draw_weight(key_w, rows_out, cols_in):
    key_bulk, key_left, key_right = jax.random.split(key_w, 3)
    bulk_part = jax.random.normal(key_bulk, (rows_out, cols_in), jnp.float32) * cols_in ** -0.5
    left_vec = jax.random.normal(key_left, (rows_out,), jnp.float32)
    left_vec = left_vec / jnp.sqrt(jnp.sum(left_vec * left_vec))
    right_vec = jax.random.normal(key_right, (cols_in,), jnp.float32)
    right_vec = right_vec / jnp.sqrt(jnp.sum(right_vec * right_vec))
    strength = 1.5 * (1.0 + (rows_out / cols_in) ** 0.5)
    weight = bulk_part + strength * left_vec[:, None] * right_vec[None, :]
    return weight.astype(jnp.bfloat16), left_vec


def draw_u(key_u, left_vec, cosine):
    other_vec = jax.random.normal(key_u, left_vec.shape, jnp.float32)
    other_vec = other_vec - jnp.sum(other_vec * left_vec) * left_vec
    other_vec = other_vec / jnp.sqrt(jnp.sum(other_vec * other_vec))
    return cosine * left_vec + (1.0 - cosine * cosine) ** 0.5 * other_vec


def power_step(weight, u_vec):
    w_full = weight.astype(jnp.float32)
    p_vec = jnp.dot(u_vec, w_full)
    v_vec = p_vec / jnp.maximum(jnp.sqrt(jnp.sum(p_vec * p_vec)), 1e-12)
    s_vec = jnp.dot(w_full, v_vec)
    sigma_val = jnp.sqrt(jnp.sum(s_vec * s_vec))
    return s_vec / sigma_val, v_vec, sigma_val


def forward_stack(x_in, weights, u_vecs):
    saved_in = []
    saved_out = []
    layer_stats = []
    for layer_idx in range(3):
        if layer_idx == 0:
            layer_in = x_in
        else:
            layer_in = jax.nn.leaky_relu(saved_out[-1], 0.2).astype(jnp.bfloat16)
        u_next, v_vec, sigma_val = power_step(weights[layer_idx], u_vecs[layer_idx])
        y_val = jnp.dot(layer_in, weights[layer_idx].T, preferred_element_type=jnp.float32) / sigma_val
        saved_in.append(layer_in)
        saved_out.append(y_val)
        layer_stats.append((u_next, v_vec, sigma_val))
    return saved_in, saved_out, layer_stats


def setup_inputs(seed: int = 0, part: int = 0) -> dict:
    key_part = jax.random.fold_in(jax.random.key(seed), part)
    key_list = jax.random.split(key_part, 8)
    w_in, left_in = draw_weight(key_list[0], HIDDEN_DIM, MODEL_DIM)
    w_mid, left_mid = draw_weight(key_list[1], HIDDEN_DIM, HIDDEN_DIM)
    w_out, left_out = draw_weight(key_list[2], MODEL_DIM, HIDDEN_DIM)
    u_in = draw_u(key_list[3], left_in, 0.65)
    u_mid = draw_u(key_list[4], left_mid, 0.7)
    u_out = draw_u(key_list[5], left_out, 0.6)
    x_in = jax.random.normal(key_list[6], (BATCH_ROWS, MODEL_DIM), jnp.float32).astype(jnp.bfloat16)
    y_last = forward_stack(x_in, [w_in, w_mid, w_out], [u_in, u_mid, u_out])[1][2]
    y_scale = jnp.sqrt(jnp.mean(y_last * y_last))
    noise_part = jax.random.normal(key_list[7], (BATCH_ROWS, MODEL_DIM), jnp.float32)
    target = (0.6 * y_last + 0.8 * y_scale * noise_part).astype(jnp.bfloat16)
    return {"x_in": x_in, "w_in": w_in, "w_mid": w_mid, "w_out": w_out, "u_in": u_in, "u_mid": u_mid, "u_out": u_out, "target": target}


def reference(x_in, w_in, w_mid, w_out, u_in, u_mid, u_out, target):
    weights = [w_in, w_mid, w_out]
    saved_in, saved_out, layer_stats = forward_stack(x_in, weights, [u_in, u_mid, u_out])
    residual = saved_out[2] - target.astype(jnp.float32)
    loss_val = 0.5 / BATCH_ROWS * jnp.sum(residual * residual)
    grad_y = residual / BATCH_ROWS
    grads_w = [None, None, None]
    for layer_idx in (2, 1, 0):
        u_next, v_vec, sigma_val = layer_stats[layer_idx]
        grad_b = grad_y.astype(jnp.bfloat16)
        corr_sum = jnp.sum(grad_y * saved_out[layer_idx])
        g_mat = jnp.dot(grad_b.T, saved_in[layer_idx], preferred_element_type=jnp.float32)
        grads_w[layer_idx] = g_mat / sigma_val - (corr_sum / sigma_val) * jnp.outer(u_next, v_vec)
        grad_x = (jnp.dot(grad_b, weights[layer_idx], preferred_element_type=jnp.float32) / sigma_val).astype(jnp.bfloat16)
        if layer_idx > 0:
            grad_y = grad_x.astype(jnp.float32) * jnp.where(saved_out[layer_idx - 1] > 0, 1.0, 0.2)
    return (loss_val.reshape(1), grad_x, grads_w[0], grads_w[1], grads_w[2],
            layer_stats[0][0], layer_stats[1][0], layer_stats[2][0],
            layer_stats[0][1], layer_stats[1][1], layer_stats[2][1],
            jnp.stack([layer_stats[0][2], layer_stats[1][2], layer_stats[2][2]]))
```

```python
import functools

import jax
import jax.numpy as jnp
from jax import lax
from jax.experimental import pallas as pl
from jax.experimental.pallas import tpu as pltpu
from jax.sharding import PartitionSpec as P

F32 = jnp.float32
BF16 = jnp.bfloat16
CORES = 2
LANES = 128
NBLK = 256
MESH_ID = pl.DeviceIdType.MESH


def wait_bytes(ref, sem):
    pltpu.make_async_copy(ref, ref, sem).wait()


def dot(a, b):
    return jnp.dot(a, b, preferred_element_type=F32)


def split3(a):
    hi = a.astype(BF16)
    rest = a - hi.astype(F32)
    mid = rest.astype(BF16)
    low = (rest - mid.astype(F32)).astype(BF16)
    return jnp.concatenate([hi, mid, low], axis=0)


def stack_kernel(n_model, chunk, batch_total,
                 w_ref, u_ref, x_hbm, t_hbm,
                 dx_hbm, dw_ref, small_ref,
                 W, WT, U, T, xb, x1, x2, y0, y1, e2, e1, e0, dxb, sums,
                 u_send, u_recv, w_send, w_fwd, w_d2d, wl, wr, wf, wp,
                 t_own, t_send, t_fwd, tl, tr, tf, tp,
                 x_sem, dx_loc, dx_send, dx_recv):
    n_chips = n_model // CORES
    n_layers, shard, width = w_ref.shape
    rows = x_hbm.shape[0] // CORES
    n_chunk = rows // chunk
    half = chunk // 2
    me = lax.axis_index("model")
    chip = me // CORES
    core = me % CORES
    right = (chip + 1) % n_chips
    left = (chip + n_chips - 1) % n_chips
    far = (chip + 2) % n_chips
    partner = chip * CORES + (1 - core)
    row0 = core * rows

    def dev(m):
        return {"model": m}

    def remote(src, dst, ssem, rsem, m):
        cp = pltpu.make_async_remote_copy(src_ref=src, dst_ref=dst, send_sem=ssem, recv_sem=rsem,
                                          device_id=dev(m), device_id_type=MESH_ID)
        cp.start()

    barrier = pltpu.get_barrier_semaphore()
    for step in range(1, n_model):
        pl.semaphore_signal(barrier, inc=1, device_id=dev((me + step) % n_model), device_id_type=MESH_ID)
    pl.semaphore_wait(barrier, n_model - 1)

    mrow = pl.multiple_of(me * shard, shard)
    hs = shard // 2

    def send_w(k):
        for nb, rsem in ((right, wl), (left, wr)):
            remote(w_ref.at[k], W.at[k, pl.ds(mrow, shard)], w_send.at[k], rsem.at[k], nb * CORES + core)
        remote(w_ref.at[k], W.at[k, pl.ds(mrow, shard)], w_d2d.at[k], wp.at[k], partner)

    def rows_of(c):
        return pl.multiple_of((c * CORES + core) * shard, shard)

    def forward_w(k):
        src_l = W.at[k, pl.ds(rows_of(left), shard)]
        src_r = W.at[k, pl.ds(rows_of(right), shard)]
        wait_bytes(src_l, wl.at[k])
        half_l = W.at[k, pl.ds(rows_of(left), hs)]
        remote(half_l, half_l, w_fwd.at[k], wf.at[k], right * CORES + core)
        remote(src_l, src_l, w_d2d.at[k], wp.at[k], partner)
        wait_bytes(src_r, wr.at[k])
        half_r = W.at[k, pl.ds(rows_of(right) + hs, hs)]
        remote(half_r, half_r, w_fwd.at[k], wf.at[k], left * CORES + core)
        remote(src_r, src_r, w_d2d.at[k], wp.at[k], partner)

    def finish_w(k):
        src_f = W.at[k, pl.ds(rows_of(far), shard)]
        wait_bytes(src_f, wf.at[k])
        remote(src_f, src_f, w_d2d.at[k], wp.at[k], partner)
        wait_bytes(W.at[k, pl.ds(0, n_chips * shard)], wp.at[k])

    def send_t(r):
        for c in range(CORES):
            src = t_hbm.at[pl.ds(c * rows + r * chunk, chunk)]
            dst = T.at[me, pl.ds(r * chunk, chunk)]
            for nb, rsem in ((right, tl), (left, tr)):
                remote(src, dst, t_send.at[r], rsem.at[r], nb * CORES + c)
        src = t_hbm.at[pl.ds(pl.multiple_of((1 - core) * rows + r * chunk, chunk), chunk)]
        remote(src, T.at[me, pl.ds(r * chunk, chunk)], t_send.at[r], tp.at[r], partner)

    def forward_t(r):
        wait_bytes(T.at[pl.ds(left * CORES, CORES), pl.ds(r * chunk, chunk)], tl.at[r])
        for c in range(CORES):
            ref = T.at[left * CORES + c, pl.ds(r * chunk, half)]
            remote(ref, ref, t_fwd.at[r], tf.at[r], right * CORES + core)
        wait_bytes(T.at[pl.ds(right * CORES, CORES), pl.ds(r * chunk, chunk)], tr.at[r])
        for c in range(CORES):
            ref = T.at[right * CORES + c, pl.ds(r * chunk + half, half)]
            remote(ref, ref, t_fwd.at[r], tf.at[r], left * CORES + core)

    def load_x(r, slot):
        return pltpu.make_async_copy(x_hbm.at[pl.ds(pl.multiple_of(row0 + r * chunk, chunk), chunk)],
                                     xb.at[slot], x_sem.at[slot])

    send_w(0)
    for step in range(1, n_model):
        remote(u_ref, U.at[me], u_send, u_recv, (me + step) % n_model)
    send_w(1)
    send_w(2)
    own_t = pltpu.make_async_copy(t_hbm.at[pl.ds(pl.multiple_of(row0, rows), rows)], T.at[me], t_own)
    own_t.start()
    load_x(0, 0).start()
    U[me] = u_ref[...]
    for k in range(n_layers):
        W[k, pl.ds(mrow, shard)] = w_ref[k]
    sums[...] = jnp.zeros_like(sums)
    dw_ref[...] = jnp.zeros_like(dw_ref)
    small_ref[...] = jnp.zeros_like(small_ref)
    wait_bytes(U.at[pl.ds(0, n_model - 1)], u_recv)
    wait_bytes(U.at[pl.ds(0, n_model - 1)], u_send)

    forward_w(0)
    for k in range(n_layers):
        if k + 1 < n_layers:
            forward_w(k + 1)
        else:
            send_t(0)
            send_t(1)
        finish_w(k)
        for i in range(width // NBLK):
            for j in range(width // NBLK):
                blk = W[k, i * NBLK:(i + 1) * NBLK, j * NBLK:(j + 1) * NBLK]
                WT[k, j * NBLK:(j + 1) * NBLK, i * NBLK:(i + 1) * NBLK] = blk.T
        u_all = jnp.concatenate([U[m] for m in range(n_model)], axis=1)
        p_all = dot(split3(u_all), W[k])
        p_row = p_all[k:k + 1] + p_all[8 + k:9 + k] + p_all[16 + k:17 + k]
        p_norm = jnp.sqrt(jnp.sum(p_row * p_row, axis=1, keepdims=True))
        v_row = p_row / jnp.maximum(p_norm, 1e-12)
        s_all = dot(split3(jnp.broadcast_to(v_row, (8, width))), WT[k])
        s_row = s_all[0:1] + s_all[8:9] + s_all[16:17]
        sigma = jnp.sqrt(jnp.sum(s_row * s_row, axis=1, keepdims=True))
        small_ref[k:k + 1] = v_row
        small_ref[n_layers + k:n_layers + k + 1] = s_row / sigma
        small_ref[2 * n_layers + k:2 * n_layers + k + 1] = jnp.broadcast_to(sigma, (1, width))
    for k in range(n_layers):
        wait_bytes(W.at[k, pl.ds(0, CORES * shard)], w_send.at[k])
        wait_bytes(W.at[k, pl.ds(0, shard)], w_fwd.at[k])
        wait_bytes(W.at[k, pl.ds(0, n_chips * shard)], w_d2d.at[k])
    own_t.wait()
    forward_t(0)
    inv = [1.0 / small_ref[2 * n_layers + k:2 * n_layers + k + 1, 0:1] for k in range(n_layers)]
    blocks = [slice(n * NBLK, (n + 1) * NBLK) for n in range(width // NBLK)]
    own_cols = pl.multiple_of(chip * CORES * shard, CORES * shard)

    def add_sum(i, val):
        sums[i] += jnp.sum(val.reshape(chunk // 8, 8, NBLK), axis=0)

    def body(r, carry):
        slot = r % 2
        load_x(r, slot).wait()

        @pl.when(r + 1 < n_chunk)
        def _():
            load_x(r + 1, 1 - slot).start()

        @pl.when(r + 2 < n_chunk)
        def _():
            send_t(r + 2)

        xin = xb.at[slot]
        for src, k, yk, xk in ((xin, 0, y0, x1), (x1, 1, y1, x2)):
            for blk in blocks:
                y_val = dot(src[...], WT[k, :, blk]) * inv[k]
                yk[:, blk] = y_val
                xk[:, blk] = jnp.maximum(y_val, 0.2 * y_val).astype(BF16)

        @pl.when(r + 1 < n_chunk)
        def _():
            forward_t(r + 1)

        wait_bytes(T.at[pl.ds(far * CORES, CORES), pl.ds(r * chunk, chunk)], tf.at[r])
        wait_bytes(T.at[partner, pl.ds(r * chunk, chunk)], tp.at[r])

        @pl.when(r >= 2)
        def _():
            out_wait(r - 2, slot)

        trow = pl.ds(pl.multiple_of(r * chunk, chunk), chunk)
        for n, blk in enumerate(blocks):
            y_val = dot(x2[...], WT[2, :, blk]) * inv[2]
            t_val = jnp.concatenate([T[2 * n, trow], T[2 * n + 1, trow]], axis=1).astype(F32)
            res = y_val - t_val
            add_sum(3, res * res)
            g_val = res / batch_total
            add_sum(2, g_val * y_val)
            e2[:, blk] = g_val.astype(BF16)
        for k, ek, yk, en in ((2, e2, y1, e1), (1, e1, y0, e0)):
            for blk in blocks:
                r_val = (dot(ek[...], W[k, :, blk]) * inv[k]).astype(BF16).astype(F32)
                y_val = yk[:, blk]
                g_val = jnp.where(y_val > 0, r_val, 0.2 * r_val)
                add_sum(k - 1, g_val * y_val)
                en[:, blk] = g_val.astype(BF16)
        for blk in blocks:
            dxb[slot, :, blk] = (dot(e0[...], W[0, :, blk]) * inv[0]).astype(BF16)
        out_copy(r, slot).start()
        out_remote(r, slot).start()
        for k, ek, xk in ((2, e2, x2), (1, e1, x1), (0, e0, xin)):
            e_own = ek[:, pl.ds(own_cols, CORES * shard)].T
            dw_ref[k] += dot(e_own, xk[...])
        return carry

    def out_rows(r):
        return pl.ds(pl.multiple_of(row0 + r * chunk, chunk), chunk)

    def out_copy(r, slot):
        return pltpu.make_async_copy(dxb.at[slot], dx_hbm.at[out_rows(r)], dx_loc.at[slot])

    def out_remote(r, slot):
        return pltpu.make_async_remote_copy(src_ref=dxb.at[slot], dst_ref=dx_hbm.at[out_rows(r)],
                                            send_sem=dx_send.at[slot], recv_sem=dx_recv.at[r],
                                            device_id=dev(partner), device_id_type=MESH_ID)

    def out_wait(r, slot):
        out_copy(r, slot).wait()
        out_remote(r, slot).wait_send()

    lax.fori_loop(0, n_chunk, body, 0)
    out_wait(n_chunk - 2, 0)
    out_wait(n_chunk - 1, 1)

    def drain(r, carry):
        wait_bytes(T.at[pl.ds(0, 2 * CORES + 1), pl.ds(0, chunk)], t_send.at[r])
        wait_bytes(T.at[pl.ds(0, CORES), pl.ds(0, chunk)], t_fwd.at[r])
        pltpu.make_async_copy(dxb.at[0], dxb.at[0], dx_recv.at[r]).wait()
        return carry

    lax.fori_loop(0, n_chunk, drain, 0)
    for i in range(4):
        tot = jnp.sum(jnp.sum(sums[i], axis=0, keepdims=True), axis=1, keepdims=True)
        small_ref[9 + i:10 + i] = jnp.broadcast_to(tot, (1, width))


def solution(mesh):
    data_size = mesh.shape["data"]
    n_model = mesh.shape["model"]
    row_spec = P(("replica", "model"), None)
    vec_spec = P(("replica", "model"))
    batch_spec = P(("replica", "data"), None)
    target_spec = P(("replica", "data"), "model")
    part_spec = P("replica")

    def local_step(x_in, w_in, w_mid, w_out, u_in, u_mid, u_out, target):
        rows_all, width = x_in.shape
        shard = w_in.shape[0]
        batch_total = rows_all * data_size
        rows = rows_all // CORES
        chunk = rows // 8
        n_chunk = rows // chunk
        w_all = jnp.stack([w_in, w_mid, w_out])
        u_all = jnp.concatenate([jnp.stack([u_in, u_mid, u_out]), jnp.zeros((5, shard), F32)], axis=0)
        vm = pltpu.VMEM
        dma = pltpu.SemaphoreType.DMA
        any_spec = pl.BlockSpec(memory_space=pl.ANY)
        vmem_spec = pl.BlockSpec(memory_space=pltpu.VMEM)
        dx, dw, small = pl.pallas_call(
            functools.partial(stack_kernel, n_model, chunk, batch_total),
            out_shape=(jax.ShapeDtypeStruct((rows_all, width), BF16),
                       jax.ShapeDtypeStruct((3, CORES * shard, width), F32),
                       jax.ShapeDtypeStruct((16, width), F32)),
            in_specs=[vmem_spec, vmem_spec, any_spec, any_spec],
            out_specs=(any_spec, vmem_spec, vmem_spec),
            scratch_shapes=[
                vm((3, width, width), BF16), vm((3, width, width), BF16),
                vm((n_model, 8, shard), F32), vm((n_model, rows, shard), BF16),
                vm((2, chunk, width), BF16), vm((chunk, width), BF16), vm((chunk, width), BF16),
                vm((chunk, width), F32), vm((chunk, width), F32),
                vm((chunk, width), BF16), vm((chunk, width), BF16), vm((chunk, width), BF16),
                vm((2, chunk, width), BF16), vm((4, 8, NBLK), F32),
                dma, dma, dma((3,)), dma((3,)), dma((3,)), dma((3,)), dma((3,)), dma((3,)), dma((3,)),
                dma, dma((n_chunk,)), dma((n_chunk,)), dma((n_chunk,)), dma((n_chunk,)), dma((n_chunk,)), dma((n_chunk,)),
                dma((2,)), dma((2,)), dma((2,)), dma((n_chunk,))],
            compiler_params=pltpu.CompilerParams(collective_id=0, has_side_effects=True,
                                                 vmem_limit_bytes=60 * 1024 * 1024),
        )(w_all, u_all, x_in, target)

        me = lax.axis_index("model")
        core = me % CORES
        v_rows = small[0:3]
        sigma = small[6:9, 0]
        scal = small[9:13, 0]
        swap = [(i, i ^ 1) for i in range(n_model)]
        mine = lax.dynamic_slice_in_dim(dw, core * shard, shard, axis=1)
        other = lax.dynamic_slice_in_dim(dw, (1 - core) * shard, shard, axis=1)
        mine = mine + lax.ppermute(other, "model", swap)
        g_mat = lax.psum(mine, "data")
        scal = lax.psum(scal, ("data", "model")) * (CORES / n_model)
        u_next = lax.dynamic_slice_in_dim(small[3:6], me * shard, shard, axis=1)
        dws = [g_mat[k] / sigma[k] - (scal[k] / sigma[k]) * (u_next[k][:, None] * v_rows[k][None, :]) for k in range(3)]
        loss_val = 0.5 / batch_total * scal[3]
        return (loss_val.reshape(1), dx, dws[0], dws[1], dws[2],
                u_next[0], u_next[1], u_next[2], v_rows[0], v_rows[1], v_rows[2], sigma)

    in_specs = (batch_spec, row_spec, row_spec, row_spec, vec_spec, vec_spec, vec_spec, target_spec)
    out_specs = (part_spec, batch_spec, row_spec, row_spec, row_spec, vec_spec, vec_spec, vec_spec, part_spec, part_spec, part_spec, part_spec)
    return jax.shard_map(local_step, mesh=mesh, in_specs=in_specs, out_specs=out_specs, check_vma=False)
```

```python
import functools

import jax
import jax.numpy as jnp
from jax import lax
from jax.experimental import pallas as pl
from jax.experimental.pallas import tpu as pltpu
from jax.sharding import PartitionSpec as P

F32 = jnp.float32
BF16 = jnp.bfloat16
CORES = 2
LANES = 128
NBLK = 256
MESH_ID = pl.DeviceIdType.MESH


def wait_bytes(ref, sem):
    pltpu.make_async_copy(ref, ref, sem).wait()


def dot(a, b):
    return jnp.dot(a, b, preferred_element_type=F32)


def split3(a):
    hi = a.astype(BF16)
    rest = a - hi.astype(F32)
    mid = rest.astype(BF16)
    low = (rest - mid.astype(F32)).astype(BF16)
    return jnp.concatenate([hi, mid, low], axis=0)


def stack_kernel(n_model, n_data, chunk, batch_total,
                 w_ref, u_ref, x_hbm, t_hbm,
                 dx_hbm, g_ref, small_ref,
                 dw_ref, pair, far_l, far_r, near_l, near_r, tiles, W, WT, U, T, xb, x1, x2, y0, y1, e2, e1, e0, dxb, sums,
                 u_send, u_recv, w_send, w_fwd, w_d2d, wl, wr, wf, wp,
                 t_own, t_send, t_fwd, tl, tr, tf, tp,
                 x_sem, dx_loc, dx_send, dx_recv,
                 p_send, p_recv, fl, fr, f_send, nl, nr, n_send, gl, gr, gf, g_send, gf_send, s_send, s_recv):
    n_chips = n_model // CORES
    n_layers, shard, width = w_ref.shape
    rows = x_hbm.shape[0] // CORES
    n_chunk = rows // chunk
    half = chunk // 2
    me = lax.axis_index("model")
    chip = me // CORES
    core = me % CORES
    right = (chip + 1) % n_chips
    left = (chip + n_chips - 1) % n_chips
    far = (chip + 2) % n_chips
    partner = chip * CORES + (1 - core)
    row0 = core * rows

    def dev(m):
        return {"model": m}

    def remote(src, dst, ssem, rsem, m):
        cp = pltpu.make_async_remote_copy(src_ref=src, dst_ref=dst, send_sem=ssem, recv_sem=rsem,
                                          device_id=dev(m), device_id_type=MESH_ID)
        cp.start()

    my_data = lax.axis_index("data")

    def cell(d, m):
        return {"data": d, "model": m}

    column = [(step, c) for step in range(1, n_data) for c in (core, 1 - core)]
    barrier = pltpu.get_barrier_semaphore()
    for step in range(1, n_model):
        pl.semaphore_signal(barrier, inc=1, device_id=dev((me + step) % n_model), device_id_type=MESH_ID)
    for step, c in column:
        pl.semaphore_signal(barrier, inc=1, device_id=cell((my_data + step) % n_data, chip * CORES + c),
                            device_id_type=MESH_ID)
    pl.semaphore_wait(barrier, n_model - 1 + len(column))

    mrow = pl.multiple_of(me * shard, shard)
    hs = shard // 2

    def send_w(k):
        for nb, rsem in ((right, wl), (left, wr)):
            remote(w_ref.at[k], W.at[k, pl.ds(mrow, shard)], w_send.at[k], rsem.at[k], nb * CORES + core)
        remote(w_ref.at[k], W.at[k, pl.ds(mrow, shard)], w_d2d.at[k], wp.at[k], partner)

    def rows_of(c):
        return pl.multiple_of((c * CORES + core) * shard, shard)

    def forward_w(k):
        src_l = W.at[k, pl.ds(rows_of(left), shard)]
        src_r = W.at[k, pl.ds(rows_of(right), shard)]
        wait_bytes(src_l, wl.at[k])
        half_l = W.at[k, pl.ds(rows_of(left), hs)]
        remote(half_l, half_l, w_fwd.at[k], wf.at[k], right * CORES + core)
        remote(src_l, src_l, w_d2d.at[k], wp.at[k], partner)
        wait_bytes(src_r, wr.at[k])
        half_r = W.at[k, pl.ds(rows_of(right) + hs, hs)]
        remote(half_r, half_r, w_fwd.at[k], wf.at[k], left * CORES + core)
        remote(src_r, src_r, w_d2d.at[k], wp.at[k], partner)

    def finish_w(k):
        src_f = W.at[k, pl.ds(rows_of(far), shard)]
        wait_bytes(src_f, wf.at[k])
        remote(src_f, src_f, w_d2d.at[k], wp.at[k], partner)
        wait_bytes(W.at[k, pl.ds(0, n_chips * shard)], wp.at[k])

    def send_t(r):
        for c in range(CORES):
            src = t_hbm.at[pl.ds(c * rows + r * chunk, chunk)]
            dst = T.at[me, pl.ds(r * chunk, chunk)]
            for nb, rsem in ((right, tl), (left, tr)):
                remote(src, dst, t_send.at[r], rsem.at[r], nb * CORES + c)
        src = t_hbm.at[pl.ds(pl.multiple_of((1 - core) * rows + r * chunk, chunk), chunk)]
        remote(src, T.at[me, pl.ds(r * chunk, chunk)], t_send.at[r], tp.at[r], partner)

    def forward_t(r):
        wait_bytes(T.at[pl.ds(left * CORES, CORES), pl.ds(r * chunk, chunk)], tl.at[r])
        for c in range(CORES):
            ref = T.at[left * CORES + c, pl.ds(r * chunk, half)]
            remote(ref, ref, t_fwd.at[r], tf.at[r], right * CORES + core)
        wait_bytes(T.at[pl.ds(right * CORES, CORES), pl.ds(r * chunk, chunk)], tr.at[r])
        for c in range(CORES):
            ref = T.at[right * CORES + c, pl.ds(r * chunk + half, half)]
            remote(ref, ref, t_fwd.at[r], tf.at[r], left * CORES + core)

    def load_x(r, slot):
        return pltpu.make_async_copy(x_hbm.at[pl.ds(pl.multiple_of(row0 + r * chunk, chunk), chunk)],
                                     xb.at[slot], x_sem.at[slot])

    send_w(0)
    for step in range(1, n_model):
        remote(u_ref, U.at[me], u_send, u_recv, (me + step) % n_model)
    send_w(1)
    send_w(2)
    own_t = pltpu.make_async_copy(t_hbm.at[pl.ds(pl.multiple_of(row0, rows), rows)], T.at[me], t_own)
    own_t.start()
    load_x(0, 0).start()
    U[me] = u_ref[...]
    for k in range(n_layers):
        W[k, pl.ds(mrow, shard)] = w_ref[k]
    sums[...] = jnp.zeros_like(sums)
    dw_ref[...] = jnp.zeros_like(dw_ref)
    tiles[my_data * CORES + core] = jnp.zeros((8, LANES), F32)
    small_ref[...] = jnp.zeros_like(small_ref)
    wait_bytes(U.at[pl.ds(0, n_model - 1)], u_recv)
    wait_bytes(U.at[pl.ds(0, n_model - 1)], u_send)

    forward_w(0)
    for k in range(n_layers):
        if k + 1 < n_layers:
            forward_w(k + 1)
        else:
            send_t(0)
            send_t(1)
        finish_w(k)
        for i in range(width // NBLK):
            for j in range(width // NBLK):
                blk = W[k, i * NBLK:(i + 1) * NBLK, j * NBLK:(j + 1) * NBLK]
                WT[k, j * NBLK:(j + 1) * NBLK, i * NBLK:(i + 1) * NBLK] = blk.T
        u_all = jnp.concatenate([U[m] for m in range(n_model)], axis=1)
        p_all = dot(split3(u_all), W[k])
        p_row = p_all[k:k + 1] + p_all[8 + k:9 + k] + p_all[16 + k:17 + k]
        p_norm = jnp.sqrt(jnp.sum(p_row * p_row, axis=1, keepdims=True))
        v_row = p_row / jnp.maximum(p_norm, 1e-12)
        s_all = dot(split3(jnp.broadcast_to(v_row, (8, width))), WT[k])
        s_row = s_all[0:1] + s_all[8:9] + s_all[16:17]
        sigma = jnp.sqrt(jnp.sum(s_row * s_row, axis=1, keepdims=True))
        small_ref[k:k + 1] = v_row
        small_ref[n_layers + k:n_layers + k + 1] = s_row / sigma
        small_ref[2 * n_layers + k:2 * n_layers + k + 1] = jnp.broadcast_to(sigma, (1, width))
    for k in range(n_layers):
        wait_bytes(W.at[k, pl.ds(0, CORES * shard)], w_send.at[k])
        wait_bytes(W.at[k, pl.ds(0, shard)], w_fwd.at[k])
        wait_bytes(W.at[k, pl.ds(0, n_chips * shard)], w_d2d.at[k])
    own_t.wait()
    forward_t(0)
    inv = [1.0 / small_ref[2 * n_layers + k:2 * n_layers + k + 1, 0:1] for k in range(n_layers)]
    blocks = [slice(n * NBLK, (n + 1) * NBLK) for n in range(width // NBLK)]
    own_cols = pl.multiple_of(chip * CORES * shard, CORES * shard)

    def add_sum(i, val):
        sums[i] += jnp.sum(val.reshape(chunk // 8, 8, NBLK), axis=0)

    def body(r, carry):
        slot = r % 2
        load_x(r, slot).wait()

        @pl.when(r + 1 < n_chunk)
        def _():
            load_x(r + 1, 1 - slot).start()

        @pl.when(r + 2 < n_chunk)
        def _():
            send_t(r + 2)

        xin = xb.at[slot]
        for src, k, yk, xk in ((xin, 0, y0, x1), (x1, 1, y1, x2)):
            for blk in blocks:
                y_val = dot(src[...], WT[k, :, blk]) * inv[k]
                yk[:, blk] = y_val
                xk[:, blk] = jnp.maximum(y_val, 0.2 * y_val).astype(BF16)

        @pl.when(r + 1 < n_chunk)
        def _():
            forward_t(r + 1)

        wait_bytes(T.at[pl.ds(far * CORES, CORES), pl.ds(r * chunk, chunk)], tf.at[r])
        wait_bytes(T.at[partner, pl.ds(r * chunk, chunk)], tp.at[r])

        @pl.when(r >= 2)
        def _():
            out_wait(r - 2, slot)

        trow = pl.ds(pl.multiple_of(r * chunk, chunk), chunk)
        for n, blk in enumerate(blocks):
            y_val = dot(x2[...], WT[2, :, blk]) * inv[2]
            t_val = jnp.concatenate([T[2 * n, trow], T[2 * n + 1, trow]], axis=1).astype(F32)
            res = y_val - t_val
            add_sum(3, res * res)
            g_val = res / batch_total
            add_sum(2, g_val * y_val)
            e2[:, blk] = g_val.astype(BF16)
        for k, ek, yk, en in ((2, e2, y1, e1), (1, e1, y0, e0)):
            for blk in blocks:
                r_val = (dot(ek[...], W[k, :, blk]) * inv[k]).astype(BF16).astype(F32)
                y_val = yk[:, blk]
                g_val = jnp.where(y_val > 0, r_val, 0.2 * r_val)
                add_sum(k - 1, g_val * y_val)
                en[:, blk] = g_val.astype(BF16)
        for blk in blocks:
            dxb[slot, :, blk] = (dot(e0[...], W[0, :, blk]) * inv[0]).astype(BF16)
        out_copy(r, slot).start()
        out_remote(r, slot).start()
        for k, ek, xk in ((2, e2, x2), (1, e1, x1), (0, e0, xin)):
            e_own = ek[:, pl.ds(own_cols, CORES * shard)].T
            dw_ref[k] += dot(e_own, xk[...])
        return carry

    def out_rows(r):
        return pl.ds(pl.multiple_of(row0 + r * chunk, chunk), chunk)

    def out_copy(r, slot):
        return pltpu.make_async_copy(dxb.at[slot], dx_hbm.at[out_rows(r)], dx_loc.at[slot])

    def out_remote(r, slot):
        return pltpu.make_async_remote_copy(src_ref=dxb.at[slot], dst_ref=dx_hbm.at[out_rows(r)],
                                            send_sem=dx_send.at[slot], recv_sem=dx_recv.at[r],
                                            device_id=dev(partner), device_id_type=MESH_ID)

    def out_wait(r, slot):
        out_copy(r, slot).wait()
        out_remote(r, slot).wait_send()

    lax.fori_loop(0, n_chunk, body, 0)

    for i in range(4):
        tot = jnp.sum(jnp.sum(sums[i], axis=0, keepdims=True), axis=1, keepdims=True)
        tiles[my_data * CORES + core, i:i + 1] = jnp.broadcast_to(tot, (1, LANES))
    mine = tiles.at[my_data * CORES + core]

    def remote_to(src, dst, ssem, rsem, device):
        pltpu.make_async_remote_copy(src_ref=src, dst_ref=dst, send_sem=ssem, recv_sem=rsem,
                                     device_id=device, device_id_type=MESH_ID).start()

    order = (2, 1, 0)
    mine_rows = pl.multiple_of(core * shard, shard)
    other_rows = pl.multiple_of((1 - core) * shard, shard)
    qrows = shard // n_data
    hrows = qrows // 2
    up = (my_data + 1) % n_data
    down = (my_data + n_data - 1) % n_data
    opp = (my_data + 2) % n_data
    to_up, to_down = {"data": up}, {"data": down}

    def quarter(d, off, n):
        return pl.ds(pl.multiple_of(d * qrows + off, 8), n)

    def acc_quarter(d, off, n):
        return pl.ds(pl.multiple_of(mine_rows + d * qrows + off, 8), n)

    for k in order:
        remote_to(dw_ref.at[k, pl.ds(other_rows, shard)], pair.at[k], p_send.at[k], p_recv.at[k], dev(partner))
    remote_to(mine, mine, s_send, s_recv, dev(partner))
    for step, c in column:
        remote_to(mine, mine, s_send, s_recv, cell((my_data + step) % n_data, chip * CORES + c))
    for k in order:
        wait_bytes(pair.at[k], p_recv.at[k])
        dw_ref[k, pl.ds(mine_rows, shard)] += pair[k]
        remote_to(dw_ref.at[k, acc_quarter(opp, 0, hrows)], far_l.at[k], f_send.at[k], fl.at[k], to_up)
        remote_to(dw_ref.at[k, acc_quarter(opp, hrows, hrows)], far_r.at[k], f_send.at[k], fr.at[k], to_down)
        remote_to(dw_ref.at[k, acc_quarter(up, hrows, hrows)], near_l.at[k, pl.ds(hrows, hrows)], n_send.at[k], nl.at[k], to_up)
        remote_to(dw_ref.at[k, acc_quarter(down, 0, hrows)], near_r.at[k, pl.ds(0, hrows)], n_send.at[k], nr.at[k], to_down)
    for k in order:
        wait_bytes(far_l.at[k], fl.at[k])
        dw_ref[k, acc_quarter(up, 0, hrows)] += far_l[k]
        remote_to(dw_ref.at[k, acc_quarter(up, 0, hrows)], near_l.at[k, pl.ds(0, hrows)], n_send.at[k], nl.at[k], to_up)
        wait_bytes(far_r.at[k], fr.at[k])
        dw_ref[k, acc_quarter(down, hrows, hrows)] += far_r[k]
        remote_to(dw_ref.at[k, acc_quarter(down, hrows, hrows)], near_r.at[k, pl.ds(hrows, hrows)], n_send.at[k], nr.at[k], to_down)
    for k in order:
        wait_bytes(near_l.at[k], nl.at[k])
        wait_bytes(near_r.at[k], nr.at[k])
        g_ref[k, quarter(my_data, 0, qrows)] = dw_ref[k, acc_quarter(my_data, 0, qrows)] + near_l[k] + near_r[k]
        ref = g_ref.at[k, quarter(my_data, 0, qrows)]
        remote_to(ref, ref, g_send.at[k], gl.at[k], to_up)
        remote_to(ref, ref, g_send.at[k], gr.at[k], to_down)
    for k in order:
        wait_bytes(g_ref.at[k, quarter(down, 0, qrows)], gl.at[k])
        ref = g_ref.at[k, quarter(down, 0, hrows)]
        remote_to(ref, ref, gf_send.at[k], gf.at[k], to_up)
        wait_bytes(g_ref.at[k, quarter(up, 0, qrows)], gr.at[k])
        ref = g_ref.at[k, quarter(up, hrows, hrows)]
        remote_to(ref, ref, gf_send.at[k], gf.at[k], to_down)

    out_wait(n_chunk - 2, 0)
    out_wait(n_chunk - 1, 1)

    def drain(r, carry):
        wait_bytes(T.at[pl.ds(0, 2 * CORES + 1), pl.ds(0, chunk)], t_send.at[r])
        wait_bytes(T.at[pl.ds(0, CORES), pl.ds(0, chunk)], t_fwd.at[r])
        pltpu.make_async_copy(dxb.at[0], dxb.at[0], dx_recv.at[r]).wait()
        return carry

    lax.fori_loop(0, n_chunk, drain, 0)
    wait_bytes(tiles.at[pl.ds(0, len(column) + 1)], s_recv)
    wait_bytes(tiles.at[pl.ds(0, len(column) + 1)], s_send)
    total = tiles[0]
    for n in range(1, n_data * CORES):
        total = total + tiles[n]
    small_ref[9:13] = jnp.concatenate([total[0:4]] * (width // LANES), axis=1)
    for k in order:
        wait_bytes(g_ref.at[k, quarter(opp, 0, qrows)], gf.at[k])
        wait_bytes(pair.at[k], p_send.at[k])
        wait_bytes(near_l.at[k], f_send.at[k])
        wait_bytes(pair.at[k, pl.ds(0, 2 * qrows)], n_send.at[k])
        wait_bytes(pair.at[k, pl.ds(0, 2 * qrows)], g_send.at[k])
        wait_bytes(near_l.at[k], gf_send.at[k])


def solution(mesh):
    data_size = mesh.shape["data"]
    n_model = mesh.shape["model"]
    row_spec = P(("replica", "model"), None)
    vec_spec = P(("replica", "model"))
    batch_spec = P(("replica", "data"), None)
    target_spec = P(("replica", "data"), "model")
    part_spec = P("replica")

    def local_step(x_in, w_in, w_mid, w_out, u_in, u_mid, u_out, target):
        rows_all, width = x_in.shape
        shard = w_in.shape[0]
        batch_total = rows_all * data_size
        rows = rows_all // CORES
        chunk = rows // 8
        n_chunk = rows // chunk
        w_all = jnp.stack([w_in, w_mid, w_out])
        u_all = jnp.concatenate([jnp.stack([u_in, u_mid, u_out]), jnp.zeros((5, shard), F32)], axis=0)
        vm = pltpu.VMEM
        dma = pltpu.SemaphoreType.DMA
        any_spec = pl.BlockSpec(memory_space=pl.ANY)
        vmem_spec = pl.BlockSpec(memory_space=pltpu.VMEM)
        dx, g_mat, small = pl.pallas_call(
            functools.partial(stack_kernel, n_model, data_size, chunk, batch_total),
            out_shape=(jax.ShapeDtypeStruct((rows_all, width), BF16),
                       jax.ShapeDtypeStruct((3, shard, width), F32),
                       jax.ShapeDtypeStruct((16, width), F32)),
            in_specs=[vmem_spec, vmem_spec, any_spec, any_spec],
            out_specs=(any_spec, vmem_spec, vmem_spec),
            scratch_shapes=[
                vm((3, CORES * shard, width), F32), vm((3, shard, width), F32),
                vm((3, shard // data_size // 2, width), F32), vm((3, shard // data_size // 2, width), F32),
                vm((3, shard // data_size, width), F32), vm((3, shard // data_size, width), F32),
                vm((data_size * CORES, 8, LANES), F32),
                vm((3, width, width), BF16), vm((3, width, width), BF16),
                vm((n_model, 8, shard), F32), vm((n_model, rows, shard), BF16),
                vm((2, chunk, width), BF16), vm((chunk, width), BF16), vm((chunk, width), BF16),
                vm((chunk, width), F32), vm((chunk, width), F32),
                vm((chunk, width), BF16), vm((chunk, width), BF16), vm((chunk, width), BF16),
                vm((2, chunk, width), BF16), vm((4, 8, NBLK), F32),
                dma, dma, dma((3,)), dma((3,)), dma((3,)), dma((3,)), dma((3,)), dma((3,)), dma((3,)),
                dma, dma((n_chunk,)), dma((n_chunk,)), dma((n_chunk,)), dma((n_chunk,)), dma((n_chunk,)), dma((n_chunk,)),
                dma((2,)), dma((2,)), dma((2,)), dma((n_chunk,)),
                *[dma((3,)) for _ in range(13)], dma, dma],
            compiler_params=pltpu.CompilerParams(collective_id=0, has_side_effects=True,
                                                 vmem_limit_bytes=60 * 1024 * 1024),
        )(w_all, u_all, x_in, target)

        me = lax.axis_index("model")
        v_rows = small[0:3]
        sigma = small[6:9, 0]
        scal = small[9:13, 0]
        u_next = lax.dynamic_slice_in_dim(small[3:6], me * shard, shard, axis=1)
        dws = [g_mat[k] / sigma[k] - (scal[k] / sigma[k]) * (u_next[k][:, None] * v_rows[k][None, :]) for k in range(3)]
        loss_val = 0.5 / batch_total * scal[3]
        return (loss_val.reshape(1), dx, dws[0], dws[1], dws[2],
                u_next[0], u_next[1], u_next[2], v_rows[0], v_rows[1], v_rows[2], sigma)

    in_specs = (batch_spec, row_spec, row_spec, row_spec, vec_spec, vec_spec, vec_spec, target_spec)
    out_specs = (part_spec, batch_spec, row_spec, row_spec, row_spec, vec_spec, vec_spec, vec_spec, part_spec, part_spec, part_spec, part_spec)
    return jax.shard_map(local_step, mesh=mesh, in_specs=in_specs, out_specs=out_specs, check_vma=False)
```

```python
import functools

import jax
import jax.numpy as jnp
from jax import lax
from jax.experimental import pallas as pl
from jax.experimental.pallas import tpu as pltpu
from jax.sharding import PartitionSpec as P

F32 = jnp.float32
BF16 = jnp.bfloat16
CORES = 2
LANES = 128
NBLK = 256
MESH_ID = pl.DeviceIdType.MESH


def wait_bytes(ref, sem):
    pltpu.make_async_copy(ref, ref, sem).wait()


def dot(a, b):
    return jnp.dot(a, b, preferred_element_type=F32)


def split3(a):
    hi = a.astype(BF16)
    rest = a - hi.astype(F32)
    mid = rest.astype(BF16)
    low = (rest - mid.astype(F32)).astype(BF16)
    return jnp.concatenate([hi, mid, low], axis=0)


def stack_kernel(n_model, n_data, chunk, batch_total,
                 w0_ref, w1_ref, w2_ref, u0_ref, u1_ref, u2_ref, x_hbm, t_hbm,
                 dx_hbm, g_ref, small_ref,
                 dw_ref, pair, far_l, far_r, near_l, near_r, tiles, W, WT, U, T, xb, x1, x2, y0, y1, e2, e1, e0, dxb, sums,
                 u_send, u_recv, w_send, w_fwd, w_d2d, wl, wr, wf, wp,
                 t_own, t_send, t_fwd, tl, tr, tf, tp,
                 x_sem, dx_loc, dx_send, dx_recv,
                 p_send, p_recv, fl, fr, f_send, nl, nr, n_send, gl, gr, gf, g_send, gf_send, s_send, s_recv):
    n_chips = n_model // CORES
    w_refs = (w0_ref, w1_ref, w2_ref)
    n_layers = len(w_refs)
    shard, width = w0_ref.shape
    rows = x_hbm.shape[0] // CORES
    n_chunk = rows // chunk
    half = chunk // 2
    me = lax.axis_index("model")
    chip = me // CORES
    core = me % CORES
    right = (chip + 1) % n_chips
    left = (chip + n_chips - 1) % n_chips
    far = (chip + 2) % n_chips
    partner = chip * CORES + (1 - core)
    row0 = core * rows

    def dev(m):
        return {"model": m}

    def remote(src, dst, ssem, rsem, m):
        cp = pltpu.make_async_remote_copy(src_ref=src, dst_ref=dst, send_sem=ssem, recv_sem=rsem,
                                          device_id=dev(m), device_id_type=MESH_ID)
        cp.start()

    my_data = lax.axis_index("data")
    U[me] = jnp.concatenate([u0_ref[...], u1_ref[...], u2_ref[...], jnp.zeros((8 - n_layers, shard), F32)], axis=0)

    def cell(d, m):
        return {"data": d, "model": m}

    column = [(step, c) for step in range(1, n_data) for c in (core, 1 - core)]
    barrier = pltpu.get_barrier_semaphore()
    for step in range(1, n_model):
        pl.semaphore_signal(barrier, inc=1, device_id=dev((me + step) % n_model), device_id_type=MESH_ID)
    for step, c in column:
        pl.semaphore_signal(barrier, inc=1, device_id=cell((my_data + step) % n_data, chip * CORES + c),
                            device_id_type=MESH_ID)
    pl.semaphore_wait(barrier, n_model - 1 + len(column))

    mrow = pl.multiple_of(me * shard, shard)
    hs = shard // 2

    def send_w(k):
        for nb, rsem in ((right, wl), (left, wr)):
            remote(w_refs[k], W.at[k, pl.ds(mrow, shard)], w_send.at[k], rsem.at[k], nb * CORES + core)
        remote(w_refs[k], W.at[k, pl.ds(mrow, shard)], w_d2d.at[k], wp.at[k], partner)

    def rows_of(c):
        return pl.multiple_of((c * CORES + core) * shard, shard)

    def forward_w(k):
        src_l = W.at[k, pl.ds(rows_of(left), shard)]
        src_r = W.at[k, pl.ds(rows_of(right), shard)]
        wait_bytes(src_l, wl.at[k])
        half_l = W.at[k, pl.ds(rows_of(left), hs)]
        remote(half_l, half_l, w_fwd.at[k], wf.at[k], right * CORES + core)
        remote(src_l, src_l, w_d2d.at[k], wp.at[k], partner)
        wait_bytes(src_r, wr.at[k])
        half_r = W.at[k, pl.ds(rows_of(right) + hs, hs)]
        remote(half_r, half_r, w_fwd.at[k], wf.at[k], left * CORES + core)
        remote(src_r, src_r, w_d2d.at[k], wp.at[k], partner)

    def finish_w(k):
        src_f = W.at[k, pl.ds(rows_of(far), shard)]
        wait_bytes(src_f, wf.at[k])
        remote(src_f, src_f, w_d2d.at[k], wp.at[k], partner)
        wait_bytes(W.at[k, pl.ds(0, n_chips * shard)], wp.at[k])

    def send_t(r):
        for c in range(CORES):
            src = t_hbm.at[pl.ds(c * rows + r * chunk, chunk)]
            dst = T.at[me, pl.ds(r * chunk, chunk)]
            for nb, rsem in ((right, tl), (left, tr)):
                remote(src, dst, t_send.at[r], rsem.at[r], nb * CORES + c)
        src = t_hbm.at[pl.ds(pl.multiple_of((1 - core) * rows + r * chunk, chunk), chunk)]
        remote(src, T.at[me, pl.ds(r * chunk, chunk)], t_send.at[r], tp.at[r], partner)

    def forward_t(r):
        wait_bytes(T.at[pl.ds(left * CORES, CORES), pl.ds(r * chunk, chunk)], tl.at[r])
        for c in range(CORES):
            ref = T.at[left * CORES + c, pl.ds(r * chunk, half)]
            remote(ref, ref, t_fwd.at[r], tf.at[r], right * CORES + core)
        wait_bytes(T.at[pl.ds(right * CORES, CORES), pl.ds(r * chunk, chunk)], tr.at[r])
        for c in range(CORES):
            ref = T.at[right * CORES + c, pl.ds(r * chunk + half, half)]
            remote(ref, ref, t_fwd.at[r], tf.at[r], left * CORES + core)

    def load_x(r, slot):
        return pltpu.make_async_copy(x_hbm.at[pl.ds(pl.multiple_of(row0 + r * chunk, chunk), chunk)],
                                     xb.at[slot], x_sem.at[slot])

    send_w(0)
    for step in range(1, n_model):
        remote(U.at[me], U.at[me], u_send, u_recv, (me + step) % n_model)
    send_w(1)
    send_w(2)
    own_t = pltpu.make_async_copy(t_hbm.at[pl.ds(pl.multiple_of(row0, rows), rows)], T.at[me], t_own)
    own_t.start()
    load_x(0, 0).start()
    load_x(1, 1).start()
    for k in range(n_layers):
        W[k, pl.ds(mrow, shard)] = w_refs[k][...]
    sums[...] = jnp.zeros_like(sums)
    dw_ref[...] = jnp.zeros_like(dw_ref)
    tiles[my_data * CORES + core] = jnp.zeros((8, LANES), F32)
    small_ref[...] = jnp.zeros_like(small_ref)
    wait_bytes(U.at[pl.ds(0, n_model - 1)], u_recv)
    wait_bytes(U.at[pl.ds(0, n_model - 1)], u_send)

    forward_w(0)
    for k in range(n_layers):
        if k + 1 < n_layers:
            forward_w(k + 1)
        else:
            send_t(0)
            send_t(1)
        finish_w(k)
        for i in range(width // NBLK):
            for j in range(width // NBLK):
                blk = W[k, i * NBLK:(i + 1) * NBLK, j * NBLK:(j + 1) * NBLK]
                WT[k, j * NBLK:(j + 1) * NBLK, i * NBLK:(i + 1) * NBLK] = blk.T
        u_all = jnp.concatenate([U[m] for m in range(n_model)], axis=1)
        p_all = dot(split3(u_all), W[k])
        p_row = p_all[k:k + 1] + p_all[8 + k:9 + k] + p_all[16 + k:17 + k]
        p_norm = jnp.sqrt(jnp.sum(p_row * p_row, axis=1, keepdims=True))
        v_row = p_row / jnp.maximum(p_norm, 1e-12)
        s_all = dot(split3(jnp.broadcast_to(v_row, (8, width))), WT[k])
        s_row = s_all[0:1] + s_all[8:9] + s_all[16:17]
        sigma = jnp.sqrt(jnp.sum(s_row * s_row, axis=1, keepdims=True))
        small_ref[k:k + 1] = v_row
        small_ref[n_layers + k:n_layers + k + 1] = s_row / sigma
        small_ref[2 * n_layers + k:2 * n_layers + k + 1] = jnp.broadcast_to(sigma, (1, width))
    for k in range(n_layers):
        wait_bytes(W.at[k, pl.ds(0, CORES * shard)], w_send.at[k])
        wait_bytes(W.at[k, pl.ds(0, shard)], w_fwd.at[k])
        wait_bytes(W.at[k, pl.ds(0, n_chips * shard)], w_d2d.at[k])
    own_t.wait()
    forward_t(0)
    inv = [1.0 / small_ref[2 * n_layers + k:2 * n_layers + k + 1, 0:1] for k in range(n_layers)]
    blocks = [slice(n * NBLK, (n + 1) * NBLK) for n in range(width // NBLK)]
    own_cols = pl.multiple_of(chip * CORES * shard, CORES * shard)
    subs = [pl.ds(h * chunk, chunk) for h in range(2)]

    def fold(val):
        return jnp.sum(val.reshape(chunk // 8, 8, NBLK), axis=0)

    def body(i, carry):
        par = i % 2
        base = pl.multiple_of(2 * par, 2)
        for h in range(2):
            load_x(2 * i + h, base + h).wait()

        @pl.when(2 * i + 2 < n_chunk)
        def _():
            for h in range(2):
                load_x(2 * i + 2 + h, 2 - base + h).start()
            send_t(2 * i + 2)

        forward_t(2 * i + 1)
        for blk in blocks:
            for h, sub in enumerate(subs):
                y_val = dot(xb[base + h], WT[0, :, blk]) * inv[0]
                y0[sub, blk] = y_val
                x1[sub, blk] = jnp.maximum(y_val, 0.2 * y_val).astype(BF16)
        for h, sub in enumerate(subs):
            for blk in blocks:
                y_val = dot(x1[sub], WT[1, :, blk]) * inv[1]
                y1[sub, blk] = y_val
                x2[sub, blk] = jnp.maximum(y_val, 0.2 * y_val).astype(BF16)

        @pl.when(2 * i + 2 < n_chunk)
        def _():
            send_t(2 * i + 3)
            forward_t(2 * i + 2)

        for h in range(2):
            wait_bytes(T.at[pl.ds(far * CORES, CORES), pl.ds((2 * i + h) * chunk, chunk)], tf.at[2 * i + h])
            wait_bytes(T.at[partner, pl.ds((2 * i + h) * chunk, chunk)], tp.at[2 * i + h])

        loss_sum = jnp.zeros((8, NBLK), F32)
        c_sum = [jnp.zeros((8, NBLK), F32) for _ in range(n_layers)]
        for h, sub in enumerate(subs):
            trow = pl.ds(pl.multiple_of((2 * i + h) * chunk, chunk), chunk)
            for n, blk in enumerate(blocks):
                y_val = dot(x2[sub], WT[2, :, blk]) * inv[2]
                t_val = jnp.concatenate([T[2 * n, trow], T[2 * n + 1, trow]], axis=1).astype(F32)
                res = y_val - t_val
                loss_sum += fold(res * res)
                g_val = res * (1.0 / batch_total)
                c_sum[2] += fold(g_val * y_val)
                e2[sub, blk] = g_val.astype(BF16)

        def back(k, h, ek, yk, store):
            sub = subs[h]
            for blk in blocks:
                r_val = (dot(ek[sub], W[k, :, blk]) * inv[k]).astype(BF16).astype(F32)
                y_val = yk[sub, blk]
                g_val = jnp.where(y_val > 0, r_val, 0.2 * r_val)
                c_sum[k - 1] += fold(g_val * y_val)
                store(h, blk, g_val.astype(BF16))

        def store_e1(h, blk, val):
            e1[subs[h], blk] = val

        def store_e0(h, blk, val):
            e0[2 * i + h, :, blk] = val

        def weight_grad(k, e_own, x_val):
            dw_ref[k] += dot(e_own.T, x_val)

        back(2, 0, e2, y1, store_e1)
        back(2, 1, e2, y1, store_e1)
        weight_grad(2, e2[:, pl.ds(own_cols, CORES * shard)], x2[...])
        back(1, 0, e1, y0, store_e0)
        back(1, 1, e1, y0, store_e0)
        weight_grad(1, e1[:, pl.ds(own_cols, CORES * shard)], x1[...])
        for h in range(2):
            weight_grad(0, e0[2 * i + h, :, pl.ds(own_cols, CORES * shard)], xb[base + h])
        for k in range(n_layers):
            sums[k] += c_sum[k]
        sums[n_layers] += loss_sum
        return carry

    def out_rows(r):
        return pl.ds(pl.multiple_of(row0 + r * chunk, chunk), chunk)

    def out_copy(r, slot):
        return pltpu.make_async_copy(dxb.at[slot], dx_hbm.at[out_rows(r)], dx_loc.at[slot])

    def out_remote(r, slot):
        return pltpu.make_async_remote_copy(src_ref=dxb.at[slot], dst_ref=dx_hbm.at[out_rows(r)],
                                            send_sem=dx_send.at[slot], recv_sem=dx_recv.at[r],
                                            device_id=dev(partner), device_id_type=MESH_ID)

    def out_wait(r, slot):
        out_copy(r, slot).wait()
        out_remote(r, slot).wait_send()

    lax.fori_loop(0, n_chunk // 2, body, 0)

    pending = list(range(n_chunk))

    def next_dx():
        if not pending:
            return
        r = pending.pop(0)
        slot = r % 2
        if r >= 2:
            out_wait(r - 2, slot)
        for blk in blocks:
            dxb[slot, :, blk] = (dot(e0[r], W[0, :, blk]) * inv[0]).astype(BF16)
        out_copy(r, slot).start()
        out_remote(r, slot).start()


    for i in range(4):
        tot = jnp.sum(jnp.sum(sums[i], axis=0, keepdims=True), axis=1, keepdims=True)
        tiles[my_data * CORES + core, i:i + 1] = jnp.broadcast_to(tot, (1, LANES))
    mine = tiles.at[my_data * CORES + core]

    def remote_to(src, dst, ssem, rsem, device):
        pltpu.make_async_remote_copy(src_ref=src, dst_ref=dst, send_sem=ssem, recv_sem=rsem,
                                     device_id=device, device_id_type=MESH_ID).start()

    order = (2, 1, 0)
    mine_rows = pl.multiple_of(core * shard, shard)
    other_rows = pl.multiple_of((1 - core) * shard, shard)
    qrows = shard // n_data
    hrows = qrows // 2
    up = (my_data + 1) % n_data
    down = (my_data + n_data - 1) % n_data
    opp = (my_data + 2) % n_data
    to_up, to_down = {"data": up}, {"data": down}

    def quarter(d, off, n):
        return pl.ds(pl.multiple_of(d * qrows + off, 8), n)

    def acc_quarter(d, off, n):
        return pl.ds(pl.multiple_of(mine_rows + d * qrows + off, 8), n)

    for k in order:
        remote_to(dw_ref.at[k, pl.ds(other_rows, shard)], pair.at[k], p_send.at[k], p_recv.at[k], dev(partner))
    remote_to(mine, mine, s_send, s_recv, dev(partner))
    for step, c in column:
        remote_to(mine, mine, s_send, s_recv, cell((my_data + step) % n_data, chip * CORES + c))
    next_dx()
    for k in order:
        wait_bytes(pair.at[k], p_recv.at[k])
        dw_ref[k, pl.ds(mine_rows, shard)] += pair[k]
        remote_to(dw_ref.at[k, acc_quarter(opp, 0, hrows)], far_l.at[k], f_send.at[k], fl.at[k], to_up)
        remote_to(dw_ref.at[k, acc_quarter(opp, hrows, hrows)], far_r.at[k], f_send.at[k], fr.at[k], to_down)
        remote_to(dw_ref.at[k, acc_quarter(up, hrows, hrows)], near_l.at[k, pl.ds(hrows, hrows)], n_send.at[k], nl.at[k], to_up)
        remote_to(dw_ref.at[k, acc_quarter(down, 0, hrows)], near_r.at[k, pl.ds(0, hrows)], n_send.at[k], nr.at[k], to_down)
    next_dx()
    for k in order:
        next_dx()
        wait_bytes(far_l.at[k], fl.at[k])
        dw_ref[k, acc_quarter(up, 0, hrows)] += far_l[k]
        remote_to(dw_ref.at[k, acc_quarter(up, 0, hrows)], near_l.at[k, pl.ds(0, hrows)], n_send.at[k], nl.at[k], to_up)
        wait_bytes(far_r.at[k], fr.at[k])
        dw_ref[k, acc_quarter(down, hrows, hrows)] += far_r[k]
        remote_to(dw_ref.at[k, acc_quarter(down, hrows, hrows)], near_r.at[k, pl.ds(hrows, hrows)], n_send.at[k], nr.at[k], to_down)
    for k in order:
        next_dx()
        wait_bytes(near_l.at[k], nl.at[k])
        wait_bytes(near_r.at[k], nr.at[k])
        g_ref[k, quarter(my_data, 0, qrows)] = dw_ref[k, acc_quarter(my_data, 0, qrows)] + near_l[k] + near_r[k]
        ref = g_ref.at[k, quarter(my_data, 0, qrows)]
        remote_to(ref, ref, g_send.at[k], gl.at[k], to_up)
        remote_to(ref, ref, g_send.at[k], gr.at[k], to_down)
    for k in order:
        wait_bytes(g_ref.at[k, quarter(down, 0, qrows)], gl.at[k])
        ref = g_ref.at[k, quarter(down, 0, hrows)]
        remote_to(ref, ref, gf_send.at[k], gf.at[k], to_up)
        wait_bytes(g_ref.at[k, quarter(up, 0, qrows)], gr.at[k])
        ref = g_ref.at[k, quarter(up, hrows, hrows)]
        remote_to(ref, ref, gf_send.at[k], gf.at[k], to_down)

    while pending:
        next_dx()
    out_wait(n_chunk - 2, 0)
    out_wait(n_chunk - 1, 1)

    def drain(r, carry):
        wait_bytes(T.at[pl.ds(0, 2 * CORES + 1), pl.ds(0, chunk)], t_send.at[r])
        wait_bytes(T.at[pl.ds(0, CORES), pl.ds(0, chunk)], t_fwd.at[r])
        pltpu.make_async_copy(dxb.at[0], dxb.at[0], dx_recv.at[r]).wait()
        return carry

    lax.fori_loop(0, n_chunk, drain, 0)
    wait_bytes(tiles.at[pl.ds(0, len(column) + 1)], s_recv)
    wait_bytes(tiles.at[pl.ds(0, len(column) + 1)], s_send)
    total = tiles[0]
    for n in range(1, n_data * CORES):
        total = total + tiles[n]
    small_ref[9:13] = jnp.concatenate([total[0:4]] * (width // LANES), axis=1)
    for k in order:
        wait_bytes(g_ref.at[k, quarter(opp, 0, qrows)], gf.at[k])
        wait_bytes(pair.at[k], p_send.at[k])
        wait_bytes(near_l.at[k], f_send.at[k])
        wait_bytes(pair.at[k, pl.ds(0, 2 * qrows)], n_send.at[k])
        wait_bytes(pair.at[k, pl.ds(0, 2 * qrows)], g_send.at[k])
        wait_bytes(near_l.at[k], gf_send.at[k])


def finish_kernel(batch_total, dx_in, g_ref, small_ref, dx_out, loss_ref, dw0, dw1, dw2,
                  un0, un1, un2, v0, v1, v2, sig_ref, buf, in_sem, out_sem):
    n_layers, shard, width = g_ref.shape
    slots, rows, _ = buf.shape
    me = lax.axis_index("model")
    loads = [pltpu.make_async_copy(dx_in.at[pl.ds(n * rows, rows)], buf.at[n], in_sem.at[n]) for n in range(slots)]
    stores = [pltpu.make_async_copy(buf.at[n], dx_out.at[pl.ds(n * rows, rows)], out_sem.at[n]) for n in range(slots)]
    for load in loads:
        load.start()
    mine = pl.ds(pl.multiple_of(me * shard, shard), shard)
    sigs = []
    for k, (dw, un, v) in enumerate(((dw0, un0, v0), (dw1, un1, v1), (dw2, un2, v2))):
        v_row = small_ref[k:k + 1]
        u_row = small_ref[n_layers + k:n_layers + k + 1, mine]
        sigma = small_ref[2 * n_layers + k:2 * n_layers + k + 1, 0:1]
        scale = small_ref[3 * n_layers + k:3 * n_layers + k + 1, 0:1] / sigma
        u_col = jnp.broadcast_to(u_row, (8, shard)).T[:, 0:1]
        dw[...] = g_ref[k] * (1.0 / sigma) - (scale * u_col) * v_row
        un[...] = u_row
        v[...] = v_row
        sigs.append(sigma)
    sig_ref[...] = jnp.concatenate(sigs, axis=1)
    loss_ref[...] = (0.5 / batch_total) * small_ref[4 * n_layers:4 * n_layers + 1, 0:1]
    for load, store in zip(loads, stores):
        load.wait()
        store.start()
    for store in stores:
        store.wait()


def solution(mesh):
    data_size = mesh.shape["data"]
    n_model = mesh.shape["model"]
    row_spec = P(("replica", "model"), None)
    vec_spec = P(("replica", "model"))
    batch_spec = P(("replica", "data"), None)
    target_spec = P(("replica", "data"), "model")
    part_spec = P("replica")

    def local_step(x_in, w_in, w_mid, w_out, u_in, u_mid, u_out, target):
        rows_all, width = x_in.shape
        shard = w_in.shape[0]
        batch_total = rows_all * data_size
        rows = rows_all // CORES
        chunk = rows // 8
        n_chunk = rows // chunk
        vm = pltpu.VMEM
        dma = pltpu.SemaphoreType.DMA
        any_spec = pl.BlockSpec(memory_space=pl.ANY)
        vmem_spec = pl.BlockSpec(memory_space=pltpu.VMEM)
        dx, g_mat, small = pl.pallas_call(
            functools.partial(stack_kernel, n_model, data_size, chunk, batch_total),
            out_shape=(jax.ShapeDtypeStruct((rows_all, width), BF16),
                       jax.ShapeDtypeStruct((3, shard, width), F32),
                       jax.ShapeDtypeStruct((16, width), F32)),
            in_specs=[vmem_spec] * 6 + [any_spec, any_spec],
            out_specs=(any_spec, vmem_spec, vmem_spec),
            scratch_shapes=[
                vm((3, CORES * shard, width), F32), vm((3, shard, width), F32),
                vm((3, shard // data_size // 2, width), F32), vm((3, shard // data_size // 2, width), F32),
                vm((3, shard // data_size, width), F32), vm((3, shard // data_size, width), F32),
                vm((data_size * CORES, 8, LANES), F32),
                vm((3, width, width), BF16), vm((3, width, width), BF16),
                vm((n_model, 8, shard), F32), vm((n_model, rows, shard), BF16),
                vm((4, chunk, width), BF16), vm((2 * chunk, width), BF16), vm((2 * chunk, width), BF16),
                vm((2 * chunk, width), F32), vm((2 * chunk, width), F32),
                vm((2 * chunk, width), BF16), vm((2 * chunk, width), BF16), vm((n_chunk, chunk, width), BF16),
                vm((2, chunk, width), BF16), vm((4, 8, NBLK), F32),
                dma, dma, dma((3,)), dma((3,)), dma((3,)), dma((3,)), dma((3,)), dma((3,)), dma((3,)),
                dma, dma((n_chunk,)), dma((n_chunk,)), dma((n_chunk,)), dma((n_chunk,)), dma((n_chunk,)), dma((n_chunk,)),
                dma((4,)), dma((2,)), dma((2,)), dma((n_chunk,)),
                *[dma((3,)) for _ in range(13)], dma, dma],
            compiler_params=pltpu.CompilerParams(collective_id=0, has_side_effects=True,
                                                 vmem_limit_bytes=67043328),
        )(w_in, w_mid, w_out, u_in.reshape(1, shard), u_mid.reshape(1, shard), u_out.reshape(1, shard), x_in, target)

        slots = 16
        sds = jax.ShapeDtypeStruct
        outs = pl.pallas_call(
            functools.partial(finish_kernel, batch_total),
            out_shape=([sds((rows_all, width), BF16), sds((1, 1), F32)] + [sds((shard, width), F32)] * 3
                       + [sds((1, shard), F32)] * 3 + [sds((1, width), F32)] * 3 + [sds((1, 3), F32)]),
            in_specs=[any_spec, vmem_spec, vmem_spec],
            out_specs=[any_spec] + [vmem_spec] * 11,
            scratch_shapes=[vm((slots, rows_all // slots, width), BF16), dma((slots,)), dma((slots,))],
        )(dx, g_mat, small)
        return (outs[1].reshape(1), outs[0], outs[2], outs[3], outs[4]) + tuple(o.reshape(-1) for o in outs[5:])

    in_specs = (batch_spec, row_spec, row_spec, row_spec, vec_spec, vec_spec, vec_spec, target_spec)
    out_specs = (part_spec, batch_spec, row_spec, row_spec, row_spec, vec_spec, vec_spec, vec_spec, part_spec, part_spec, part_spec, part_spec)
    return jax.shard_map(local_step, mesh=mesh, in_specs=in_specs, out_specs=out_specs, check_vma=False)
```

```python
import functools

import jax
import jax.numpy as jnp
from jax import lax
from jax.experimental import pallas as pl
from jax.experimental.pallas import tpu as pltpu
from jax.sharding import PartitionSpec as P

F32 = jnp.float32
BF16 = jnp.bfloat16
CORES = 2
LANES = 128
NBLK = 256
MESH_ID = pl.DeviceIdType.MESH


def wait_bytes(ref, sem):
    pltpu.make_async_copy(ref, ref, sem).wait()


def dot(a, b):
    return jnp.dot(a, b, preferred_element_type=F32)


def split3(a):
    hi = a.astype(BF16)
    rest = a - hi.astype(F32)
    mid = rest.astype(BF16)
    low = (rest - mid.astype(F32)).astype(BF16)
    return jnp.concatenate([hi, mid, low], axis=0)


def stack_kernel(n_model, n_data, chunk, batch_total,
                 w0_ref, w1_ref, w2_ref, u0_ref, u1_ref, u2_ref, x_hbm, t_hbm,
                 dx_hbm, g_ref, small_ref,
                 dw_ref, pair, far_l, far_r, near_l, near_r, tiles, W, WT, U, T, xb, x1, x2, y0, y1, e2, e1, e0, dxb, sums,
                 u_send, u_recv, w_send, w_fwd, w_d2d, wl, wr, wf, wp, wy_send, wy_up, wy_down, wy_far,
                 t_own, t_send, t_fwd, tl, tr, tf, tp,
                 x_sem, dx_loc, dx_send, dx_recv,
                 p_send, p_recv, fl, fr, f_send, nl, nr, n_send, gl, gr, gf, g_send, gf_send, s_send, s_recv):
    n_chips = n_model // CORES
    w_refs = (w0_ref, w1_ref, w2_ref)
    n_layers = len(w_refs)
    shard, width = w0_ref.shape
    rows = x_hbm.shape[0] // CORES
    n_chunk = rows // chunk
    half = chunk // 2
    me = lax.axis_index("model")
    chip = me // CORES
    core = me % CORES
    right = (chip + 1) % n_chips
    left = (chip + n_chips - 1) % n_chips
    far = (chip + 2) % n_chips
    partner = chip * CORES + (1 - core)
    row0 = core * rows

    def dev(m):
        return {"model": m}

    def remote(src, dst, ssem, rsem, m):
        cp = pltpu.make_async_remote_copy(src_ref=src, dst_ref=dst, send_sem=ssem, recv_sem=rsem,
                                          device_id=dev(m), device_id_type=MESH_ID)
        cp.start()

    my_data = lax.axis_index("data")
    U[me] = jnp.concatenate([u0_ref[...], u1_ref[...], u2_ref[...], jnp.zeros((8 - n_layers, shard), F32)], axis=0)

    def cell(d, m):
        return {"data": d, "model": m}

    column = [(step, c) for step in range(1, n_data) for c in (core, 1 - core)]
    barrier = pltpu.get_barrier_semaphore()
    for step in range(1, n_model):
        pl.semaphore_signal(barrier, inc=1, device_id=dev((me + step) % n_model), device_id_type=MESH_ID)
    for step, c in column:
        pl.semaphore_signal(barrier, inc=1, device_id=cell((my_data + step) % n_data, chip * CORES + c),
                            device_id_type=MESH_ID)
    pl.semaphore_wait(barrier, n_model - 1 + len(column))

    mrow = pl.multiple_of(me * shard, shard)
    hs = shard // 2

    def send_w(k):
        for nb, rsem in ((right, wl), (left, wr)):
            remote(w_refs[k], W.at[k, pl.ds(mrow, shard)], w_send.at[k], rsem.at[k], nb * CORES + core)
        remote(w_refs[k], W.at[k, pl.ds(mrow, shard)], w_d2d.at[k], wp.at[k], partner)

    def rows_of(c):
        return pl.multiple_of((c * CORES + core) * shard, shard)

    def forward_w(k):
        src_l = W.at[k, pl.ds(rows_of(left), shard)]
        src_r = W.at[k, pl.ds(rows_of(right), shard)]
        wait_bytes(src_l, wl.at[k])
        half_l = W.at[k, pl.ds(rows_of(left), hs)]
        remote(half_l, half_l, w_fwd.at[k], wf.at[k], right * CORES + core)
        remote(src_l, src_l, w_d2d.at[k], wp.at[k], partner)
        wait_bytes(src_r, wr.at[k])
        half_r = W.at[k, pl.ds(rows_of(right) + hs, hs)]
        remote(half_r, half_r, w_fwd.at[k], wf.at[k], left * CORES + core)
        remote(src_r, src_r, w_d2d.at[k], wp.at[k], partner)

    def finish_w(k):
        src_f = W.at[k, pl.ds(rows_of(far), shard)]
        wait_bytes(src_f, wf.at[k])
        remote(src_f, src_f, w_d2d.at[k], wp.at[k], partner)
        wait_bytes(W.at[k, pl.ds(0, n_chips * shard)], wp.at[k])

    qrows = shard // n_data
    hrows = qrows // 2
    up = (my_data + 1) % n_data
    down = (my_data + n_data - 1) % n_data
    opp = (my_data + 2) % n_data
    to_up, to_down = {"data": up}, {"data": down}

    def w_part(k, c, d, off, n):
        return W.at[k, pl.ds(pl.multiple_of((c * CORES + core) * shard + d * qrows + off, hrows), n)]

    def remote_to(src, dst, ssem, rsem, device):
        pltpu.make_async_remote_copy(src_ref=src, dst_ref=dst, send_sem=ssem, recv_sem=rsem,
                                     device_id=device, device_id_type=MESH_ID).start()

    def send_wq(k):
        src = w_refs[k].at[pl.ds(pl.multiple_of(my_data * qrows, qrows), qrows)]
        for nb, rsem in ((right, wl), (left, wr), (far, wf)):
            remote(src, w_part(k, chip, my_data, 0, qrows), w_send.at[k], rsem.at[k], nb * CORES + core)
        remote(w_refs[k], W.at[k, pl.ds(mrow, shard)], w_d2d.at[k], wp.at[k], partner)

    def spread_wq(k):
        for c, rsem in ((left, wl), (right, wr), (far, wf)):
            ref = w_part(k, c, my_data, 0, qrows)
            wait_bytes(ref, rsem.at[k])
            remote_to(ref, ref, wy_send.at[k], wy_down.at[k], to_up)
            remote_to(ref, ref, wy_send.at[k], wy_up.at[k], to_down)

    def relay_wq(k):
        wait_bytes(W.at[k, pl.ds(0, 3 * qrows)], wy_down.at[k])
        for c in (left, right, far):
            ref = w_part(k, c, down, 0, hrows)
            remote_to(ref, ref, w_fwd.at[k], wy_far.at[k], to_up)
        wait_bytes(W.at[k, pl.ds(0, 3 * qrows)], wy_up.at[k])
        for c in (left, right, far):
            ref = w_part(k, c, up, hrows, hrows)
            remote_to(ref, ref, w_fwd.at[k], wy_far.at[k], to_down)

    def finish_wq(k):
        wait_bytes(W.at[k, pl.ds(0, 3 * qrows)], wy_far.at[k])
        for c in (left, right, far):
            ref = W.at[k, pl.ds(rows_of(c), shard)]
            remote(ref, ref, w_d2d.at[k], wp.at[k], partner)
        wait_bytes(W.at[k, pl.ds(0, n_chips * shard)], wp.at[k])

    def send_t(r):
        for c in range(CORES):
            src = t_hbm.at[pl.ds(c * rows + r * chunk, chunk)]
            dst = T.at[me, pl.ds(r * chunk, chunk)]
            for nb, rsem in ((right, tl), (left, tr)):
                remote(src, dst, t_send.at[r], rsem.at[r], nb * CORES + c)
        src = t_hbm.at[pl.ds(pl.multiple_of((1 - core) * rows + r * chunk, chunk), chunk)]
        remote(src, T.at[me, pl.ds(r * chunk, chunk)], t_send.at[r], tp.at[r], partner)

    def forward_t(r):
        wait_bytes(T.at[pl.ds(left * CORES, CORES), pl.ds(r * chunk, chunk)], tl.at[r])
        for c in range(CORES):
            ref = T.at[left * CORES + c, pl.ds(r * chunk, half)]
            remote(ref, ref, t_fwd.at[r], tf.at[r], right * CORES + core)
        wait_bytes(T.at[pl.ds(right * CORES, CORES), pl.ds(r * chunk, chunk)], tr.at[r])
        for c in range(CORES):
            ref = T.at[right * CORES + c, pl.ds(r * chunk + half, half)]
            remote(ref, ref, t_fwd.at[r], tf.at[r], left * CORES + core)

    def load_x(r, slot):
        return pltpu.make_async_copy(x_hbm.at[pl.ds(pl.multiple_of(row0 + r * chunk, chunk), chunk)],
                                     xb.at[slot], x_sem.at[slot])

    send_wq(1)
    send_wq(2)
    send_w(0)
    for step in range(1, n_model):
        remote(U.at[me], U.at[me], u_send, u_recv, (me + step) % n_model)
    send_t(0)
    own_t = pltpu.make_async_copy(t_hbm.at[pl.ds(pl.multiple_of(row0, rows), rows)], T.at[me], t_own)
    own_t.start()
    load_x(0, 0).start()
    load_x(1, 1).start()
    for k in range(n_layers):
        W[k, pl.ds(mrow, shard)] = w_refs[k][...]
    sums[...] = jnp.zeros_like(sums)
    dw_ref[...] = jnp.zeros_like(dw_ref)
    tiles[my_data * CORES + core] = jnp.zeros((8, LANES), F32)
    small_ref[...] = jnp.zeros_like(small_ref)
    spread_wq(1)
    spread_wq(2)
    wait_bytes(U.at[pl.ds(0, n_model - 1)], u_recv)
    wait_bytes(U.at[pl.ds(0, n_model - 1)], u_send)
    forward_w(0)
    send_t(1)
    relay_wq(1)
    for k in range(n_layers):
        if k == 0:
            finish_w(0)
        else:
            if k == 2:
                send_t(2)
            finish_wq(k)
        for i in range(width // NBLK):
            for j in range(width // NBLK):
                blk = W[k, i * NBLK:(i + 1) * NBLK, j * NBLK:(j + 1) * NBLK]
                WT[k, j * NBLK:(j + 1) * NBLK, i * NBLK:(i + 1) * NBLK] = blk.T
        u_all = jnp.concatenate([U[m] for m in range(n_model)], axis=1)
        p_all = dot(split3(u_all), W[k])
        p_row = p_all[k:k + 1] + p_all[8 + k:9 + k] + p_all[16 + k:17 + k]
        p_norm = jnp.sqrt(jnp.sum(p_row * p_row, axis=1, keepdims=True))
        v_row = p_row / jnp.maximum(p_norm, 1e-12)
        s_all = dot(split3(jnp.broadcast_to(v_row, (8, width))), WT[k])
        s_row = s_all[0:1] + s_all[8:9] + s_all[16:17]
        sigma = jnp.sqrt(jnp.sum(s_row * s_row, axis=1, keepdims=True))
        small_ref[k:k + 1] = v_row
        small_ref[n_layers + k:n_layers + k + 1] = s_row / sigma
        small_ref[2 * n_layers + k:2 * n_layers + k + 1] = jnp.broadcast_to(sigma, (1, width))
        if k == 0:
            relay_wq(2)
    for k in range(n_layers):
        wait_bytes(W.at[k, pl.ds(0, 3 * qrows if k else CORES * shard)], w_send.at[k])
        wait_bytes(W.at[k, pl.ds(0, 6 * hrows if k else shard)], w_fwd.at[k])
        if k:
            wait_bytes(W.at[k, pl.ds(0, 6 * qrows)], wy_send.at[k])
        wait_bytes(W.at[k, pl.ds(0, n_chips * shard)], w_d2d.at[k])
    own_t.wait()
    inv = [1.0 / small_ref[2 * n_layers + k:2 * n_layers + k + 1, 0:1] for k in range(n_layers)]
    blocks = [slice(n * NBLK, (n + 1) * NBLK) for n in range(width // NBLK)]
    own_cols = pl.multiple_of(chip * CORES * shard, CORES * shard)
    subs = [pl.ds(h * chunk, chunk) for h in range(2)]

    def fold(val):
        return jnp.sum(val.reshape(chunk // 8, 8, NBLK), axis=0)

    def body(i, carry):
        par = i % 2
        base = pl.multiple_of(2 * par, 2)
        for h in range(2):
            load_x(2 * i + h, base + h).wait()

        forward_t(2 * i)
        forward_t(2 * i + 1)

        @pl.when(2 * i + 2 < n_chunk)
        def _():
            for h in range(2):
                load_x(2 * i + 2 + h, 2 - base + h).start()
            send_t(2 * i + 3)

        @pl.when(2 * i + 4 < n_chunk)
        def _():
            send_t(2 * i + 4)

        for blk in blocks:
            for h, sub in enumerate(subs):
                y_val = dot(xb[base + h], WT[0, :, blk]) * inv[0]
                y0[sub, blk] = y_val
                x1[sub, blk] = jnp.maximum(y_val, 0.2 * y_val).astype(BF16)
        for h, sub in enumerate(subs):
            for blk in blocks:
                y_val = dot(x1[sub], WT[1, :, blk]) * inv[1]
                y1[sub, blk] = y_val
                x2[sub, blk] = jnp.maximum(y_val, 0.2 * y_val).astype(BF16)

        loss_sum = jnp.zeros((8, NBLK), F32)
        c_sum = [jnp.zeros((8, NBLK), F32) for _ in range(n_layers)]
        for h, sub in enumerate(subs):
            wait_bytes(T.at[pl.ds(far * CORES, CORES), pl.ds((2 * i + h) * chunk, chunk)], tf.at[2 * i + h])
            wait_bytes(T.at[partner, pl.ds((2 * i + h) * chunk, chunk)], tp.at[2 * i + h])
            trow = pl.ds(pl.multiple_of((2 * i + h) * chunk, chunk), chunk)
            for n, blk in enumerate(blocks):
                y_val = dot(x2[sub], WT[2, :, blk]) * inv[2]
                t_val = jnp.concatenate([T[2 * n, trow], T[2 * n + 1, trow]], axis=1).astype(F32)
                res = y_val - t_val
                loss_sum += fold(res * res)
                g_val = res * (1.0 / batch_total)
                c_sum[2] += fold(g_val * y_val)
                e2[sub, blk] = g_val.astype(BF16)

        def back(k, h, ek, yk, store):
            sub = subs[h]
            for blk in blocks:
                r_val = (dot(ek[sub], W[k, :, blk]) * inv[k]).astype(BF16).astype(F32)
                y_val = yk[sub, blk]
                g_val = jnp.where(y_val > 0, r_val, 0.2 * r_val)
                c_sum[k - 1] += fold(g_val * y_val)
                store(h, blk, g_val.astype(BF16))

        def store_e1(h, blk, val):
            e1[subs[h], blk] = val

        def store_e0(h, blk, val):
            e0[2 * i + h, :, blk] = val

        def weight_grad(k, e_own, x_val):
            dw_ref[k] += dot(e_own.T, x_val)

        back(2, 0, e2, y1, store_e1)
        back(2, 1, e2, y1, store_e1)
        weight_grad(2, e2[:, pl.ds(own_cols, CORES * shard)], x2[...])
        back(1, 0, e1, y0, store_e0)
        back(1, 1, e1, y0, store_e0)
        weight_grad(1, e1[:, pl.ds(own_cols, CORES * shard)], x1[...])
        for h in range(2):
            weight_grad(0, e0[2 * i + h, :, pl.ds(own_cols, CORES * shard)], xb[base + h])
        for k in range(n_layers):
            sums[k] += c_sum[k]
        sums[n_layers] += loss_sum
        return carry

    def out_rows(r):
        return pl.ds(pl.multiple_of(row0 + r * chunk, chunk), chunk)

    def out_copy(r, slot):
        return pltpu.make_async_copy(dxb.at[slot], dx_hbm.at[out_rows(r)], dx_loc.at[slot])

    def out_remote(r, slot):
        return pltpu.make_async_remote_copy(src_ref=dxb.at[slot], dst_ref=dx_hbm.at[out_rows(r)],
                                            send_sem=dx_send.at[slot], recv_sem=dx_recv.at[r],
                                            device_id=dev(partner), device_id_type=MESH_ID)

    def out_wait(r, slot):
        out_copy(r, slot).wait()
        out_remote(r, slot).wait_send()

    lax.fori_loop(0, n_chunk // 2, body, 0)

    pending = list(range(n_chunk))

    def next_dx():
        if not pending:
            return
        r = pending.pop(0)
        slot = r % 2
        if r >= 2:
            out_wait(r - 2, slot)
        for blk in blocks:
            dxb[slot, :, blk] = (dot(e0[r], W[0, :, blk]) * inv[0]).astype(BF16)
        out_copy(r, slot).start()
        out_remote(r, slot).start()


    for i in range(4):
        tot = jnp.sum(jnp.sum(sums[i], axis=0, keepdims=True), axis=1, keepdims=True)
        tiles[my_data * CORES + core, i:i + 1] = jnp.broadcast_to(tot, (1, LANES))
    mine = tiles.at[my_data * CORES + core]

    order = (2, 1, 0)
    mine_rows = pl.multiple_of(core * shard, shard)
    other_rows = pl.multiple_of((1 - core) * shard, shard)
    def quarter(d, off, n):
        return pl.ds(pl.multiple_of(d * qrows + off, 8), n)

    def acc_quarter(d, off, n):
        return pl.ds(pl.multiple_of(mine_rows + d * qrows + off, 8), n)

    for k in order:
        remote_to(dw_ref.at[k, pl.ds(other_rows, shard)], pair.at[k], p_send.at[k], p_recv.at[k], dev(partner))
    remote_to(mine, mine, s_send, s_recv, dev(partner))
    for step, c in column:
        remote_to(mine, mine, s_send, s_recv, cell((my_data + step) % n_data, chip * CORES + c))
    next_dx()
    for k in order:
        wait_bytes(pair.at[k], p_recv.at[k])
        dw_ref[k, pl.ds(mine_rows, shard)] += pair[k]
        remote_to(dw_ref.at[k, acc_quarter(opp, 0, hrows)], far_l.at[k], f_send.at[k], fl.at[k], to_up)
        remote_to(dw_ref.at[k, acc_quarter(opp, hrows, hrows)], far_r.at[k], f_send.at[k], fr.at[k], to_down)
        remote_to(dw_ref.at[k, acc_quarter(up, hrows, hrows)], near_l.at[k, pl.ds(hrows, hrows)], n_send.at[k], nl.at[k], to_up)
        remote_to(dw_ref.at[k, acc_quarter(down, 0, hrows)], near_r.at[k, pl.ds(0, hrows)], n_send.at[k], nr.at[k], to_down)
    next_dx()
    for k in order:
        next_dx()
        wait_bytes(far_l.at[k], fl.at[k])
        dw_ref[k, acc_quarter(up, 0, hrows)] += far_l[k]
        remote_to(dw_ref.at[k, acc_quarter(up, 0, hrows)], near_l.at[k, pl.ds(0, hrows)], n_send.at[k], nl.at[k], to_up)
        wait_bytes(far_r.at[k], fr.at[k])
        dw_ref[k, acc_quarter(down, hrows, hrows)] += far_r[k]
        remote_to(dw_ref.at[k, acc_quarter(down, hrows, hrows)], near_r.at[k, pl.ds(hrows, hrows)], n_send.at[k], nr.at[k], to_down)
    for k in order:
        next_dx()
        wait_bytes(near_l.at[k], nl.at[k])
        wait_bytes(near_r.at[k], nr.at[k])
        g_ref[k, quarter(my_data, 0, qrows)] = dw_ref[k, acc_quarter(my_data, 0, qrows)] + near_l[k] + near_r[k]
        ref = g_ref.at[k, quarter(my_data, 0, qrows)]
        remote_to(ref, ref, g_send.at[k], gl.at[k], to_up)
        remote_to(ref, ref, g_send.at[k], gr.at[k], to_down)
    for k in order:
        wait_bytes(g_ref.at[k, quarter(down, 0, qrows)], gl.at[k])
        ref = g_ref.at[k, quarter(down, 0, hrows)]
        remote_to(ref, ref, gf_send.at[k], gf.at[k], to_up)
        wait_bytes(g_ref.at[k, quarter(up, 0, qrows)], gr.at[k])
        ref = g_ref.at[k, quarter(up, hrows, hrows)]
        remote_to(ref, ref, gf_send.at[k], gf.at[k], to_down)

    while pending:
        next_dx()
    out_wait(n_chunk - 2, 0)
    out_wait(n_chunk - 1, 1)

    def drain(r, carry):
        wait_bytes(T.at[pl.ds(0, 2 * CORES + 1), pl.ds(0, chunk)], t_send.at[r])
        wait_bytes(T.at[pl.ds(0, CORES), pl.ds(0, chunk)], t_fwd.at[r])
        pltpu.make_async_copy(dxb.at[0], dxb.at[0], dx_recv.at[r]).wait()
        return carry

    lax.fori_loop(0, n_chunk, drain, 0)
    wait_bytes(tiles.at[pl.ds(0, len(column) + 1)], s_recv)
    wait_bytes(tiles.at[pl.ds(0, len(column) + 1)], s_send)
    total = tiles[0]
    for n in range(1, n_data * CORES):
        total = total + tiles[n]
    small_ref[9:13] = jnp.concatenate([total[0:4]] * (width // LANES), axis=1)
    for k in order:
        wait_bytes(g_ref.at[k, quarter(opp, 0, qrows)], gf.at[k])
        wait_bytes(pair.at[k], p_send.at[k])
        wait_bytes(near_l.at[k], f_send.at[k])
        wait_bytes(pair.at[k, pl.ds(0, 2 * qrows)], n_send.at[k])
        wait_bytes(pair.at[k, pl.ds(0, 2 * qrows)], g_send.at[k])
        wait_bytes(near_l.at[k], gf_send.at[k])


def finish_kernel(batch_total, dx_in, g_hbm, small_ref, dx_out, loss_ref, dw0, dw1, dw2,
                  un0, un1, un2, v0, v1, v2, sig_ref, buf, g_buf, d_buf, in_sem, out_sem, g_in, d_out):
    n_layers, shard, width = g_buf.shape
    slots, rows, _ = buf.shape
    me = lax.axis_index("model")
    loads = [pltpu.make_async_copy(dx_in.at[pl.ds(n * rows, rows)], buf.at[n], in_sem.at[n]) for n in range(slots)]
    stores = [pltpu.make_async_copy(buf.at[n], dx_out.at[pl.ds(n * rows, rows)], out_sem.at[n]) for n in range(slots)]
    g_load = pltpu.make_async_copy(g_hbm, g_buf, g_in)
    for load in loads[:slots // 2]:
        load.start()
    g_load.start()
    for load in loads[slots // 2:]:
        load.start()
    for load, store in zip(loads[:slots // 2], stores):
        load.wait()
        store.start()
    g_load.wait()
    mine = pl.ds(pl.multiple_of(me * shard, shard), shard)
    sigs, writes = [], []
    for k, (dw, un, v) in enumerate(((dw0, un0, v0), (dw1, un1, v1), (dw2, un2, v2))):
        v_row = small_ref[k:k + 1]
        u_row = small_ref[n_layers + k:n_layers + k + 1, mine]
        sigma = small_ref[2 * n_layers + k:2 * n_layers + k + 1, 0:1]
        scale = small_ref[3 * n_layers + k:3 * n_layers + k + 1, 0:1] / sigma
        u_col = jnp.broadcast_to(u_row, (8, shard)).T[:, 0:1]
        d_buf[k] = g_buf[k] * (1.0 / sigma) - (scale * u_col) * v_row
        writes.append(pltpu.make_async_copy(d_buf.at[k], dw, d_out.at[k]))
        un[...] = u_row
        v[...] = v_row
        sigs.append(sigma)
    sig_ref[...] = jnp.concatenate(sigs, axis=1)
    loss_ref[...] = (0.5 / batch_total) * small_ref[4 * n_layers:4 * n_layers + 1, 0:1]
    for load, store in zip(loads[slots // 2:], stores[slots // 2:]):
        load.wait()
        store.start()
    for write in writes:
        write.start()
    for copy in stores + writes:
        copy.wait()


def solution(mesh):
    data_size = mesh.shape["data"]
    n_model = mesh.shape["model"]
    row_spec = P(("replica", "model"), None)
    vec_spec = P(("replica", "model"))
    batch_spec = P(("replica", "data"), None)
    target_spec = P(("replica", "data"), "model")
    part_spec = P("replica")

    def local_step(x_in, w_in, w_mid, w_out, u_in, u_mid, u_out, target):
        rows_all, width = x_in.shape
        shard = w_in.shape[0]
        batch_total = rows_all * data_size
        rows = rows_all // CORES
        chunk = rows // 8
        n_chunk = rows // chunk
        vm = pltpu.VMEM
        dma = pltpu.SemaphoreType.DMA
        any_spec = pl.BlockSpec(memory_space=pl.ANY)
        vmem_spec = pl.BlockSpec(memory_space=pltpu.VMEM)
        dx, g_mat, small = pl.pallas_call(
            functools.partial(stack_kernel, n_model, data_size, chunk, batch_total),
            out_shape=(jax.ShapeDtypeStruct((rows_all, width), BF16),
                       jax.ShapeDtypeStruct((3, shard, width), F32),
                       jax.ShapeDtypeStruct((16, width), F32)),
            in_specs=[vmem_spec] * 6 + [any_spec, any_spec],
            out_specs=(any_spec, vmem_spec, vmem_spec),
            scratch_shapes=[
                vm((3, CORES * shard, width), F32), vm((3, shard, width), F32),
                vm((3, shard // data_size // 2, width), F32), vm((3, shard // data_size // 2, width), F32),
                vm((3, shard // data_size, width), F32), vm((3, shard // data_size, width), F32),
                vm((data_size * CORES, 8, LANES), F32),
                vm((3, width, width), BF16), vm((3, width, width), BF16),
                vm((n_model, 8, shard), F32), vm((n_model, rows, shard), BF16),
                vm((4, chunk, width), BF16), vm((2 * chunk, width), BF16), vm((2 * chunk, width), BF16),
                vm((2 * chunk, width), F32), vm((2 * chunk, width), F32),
                vm((2 * chunk, width), BF16), vm((2 * chunk, width), BF16), vm((n_chunk, chunk, width), BF16),
                vm((2, chunk, width), BF16), vm((4, 8, NBLK), F32),
                dma, dma, *[dma((3,)) for _ in range(11)],
                dma, dma((n_chunk,)), dma((n_chunk,)), dma((n_chunk,)), dma((n_chunk,)), dma((n_chunk,)), dma((n_chunk,)),
                dma((4,)), dma((2,)), dma((2,)), dma((n_chunk,)),
                *[dma((3,)) for _ in range(13)], dma, dma],
            compiler_params=pltpu.CompilerParams(collective_id=0, has_side_effects=True,
                                                 vmem_limit_bytes=67043328),
        )(w_in, w_mid, w_out, u_in.reshape(1, shard), u_mid.reshape(1, shard), u_out.reshape(1, shard), x_in, target)

        slots = 16
        sds = jax.ShapeDtypeStruct
        outs = pl.pallas_call(
            functools.partial(finish_kernel, batch_total),
            out_shape=([sds((rows_all, width), BF16), sds((1, 1), F32)] + [sds((shard, width), F32)] * 3
                       + [sds((1, shard), F32)] * 3 + [sds((1, width), F32)] * 3 + [sds((1, 3), F32)]),
            in_specs=[any_spec, any_spec, vmem_spec],
            out_specs=[any_spec, vmem_spec] + [any_spec] * 3 + [vmem_spec] * 7,
            scratch_shapes=[vm((slots, rows_all // slots, width), BF16), vm((3, shard, width), F32), vm((3, shard, width), F32),
                            dma((slots,)), dma((slots,)), dma, dma((3,))],
        )(dx, g_mat, small)
        return (outs[1].reshape(1), outs[0], outs[2], outs[3], outs[4]) + tuple(o.reshape(-1) for o in outs[5:])

    in_specs = (batch_spec, row_spec, row_spec, row_spec, vec_spec, vec_spec, vec_spec, target_spec)
    out_specs = (part_spec, batch_spec, row_spec, row_spec, row_spec, vec_spec, vec_spec, vec_spec, part_spec, part_spec, part_spec, part_spec)
    return jax.shard_map(local_step, mesh=mesh, in_specs=in_specs, out_specs=out_specs, check_vma=False)
```

```python
import functools

import jax
import jax.numpy as jnp
from jax import lax
from jax.experimental import pallas as pl
from jax.experimental.pallas import tpu as pltpu
from jax.sharding import PartitionSpec as P

F32 = jnp.float32
BF16 = jnp.bfloat16
CORES = 2
LANES = 128
NBLK = 256
MESH_ID = pl.DeviceIdType.MESH


def wait_bytes(ref, sem):
    pltpu.make_async_copy(ref, ref, sem).wait()


def dot(a, b):
    return jnp.dot(a, b, preferred_element_type=F32)


def split3(a):
    hi = a.astype(BF16)
    rest = a - hi.astype(F32)
    mid = rest.astype(BF16)
    low = (rest - mid.astype(F32)).astype(BF16)
    return jnp.concatenate([hi, mid, low], axis=0)


def stack_kernel(n_model, n_data, chunk, batch_total,
                 w0_ref, w1_ref, w2_ref, u0_ref, u1_ref, u2_ref, x_hbm, t_hbm,
                 dx_hbm, g_ref, small_ref,
                 dw_ref, pair, far_l, far_r, near_l, near_r, tiles, W, WT, U, T, xb, x1, x2, y0, y1, e2, e1, e0, dxb, sums,
                 u_send, u_recv, w_send, w_fwd, w_d2d, wl, wr, wf, wp, wy_send, wy_up, wy_down, wy_far,
                 t_own, t_send, t_fwd, tl, tr, tf, tp,
                 x_sem, dx_loc, dx_send, dx_recv,
                 p_send, p_recv, fl, fr, f_send, nl, nr, n_send, gl, gr, gf, g_send, gf_send, s_send, s_recv):
    n_chips = n_model // CORES
    w_refs = (w0_ref, w1_ref, w2_ref)
    n_layers = len(w_refs)
    shard, width = w0_ref.shape
    rows = x_hbm.shape[0] // CORES
    n_chunk = rows // chunk
    half = chunk // 2
    me = lax.axis_index("model")
    chip = me // CORES
    core = me % CORES
    right = (chip + 1) % n_chips
    left = (chip + n_chips - 1) % n_chips
    far = (chip + 2) % n_chips
    partner = chip * CORES + (1 - core)
    row0 = core * rows

    def dev(m):
        return {"model": m}

    def remote(src, dst, ssem, rsem, m):
        cp = pltpu.make_async_remote_copy(src_ref=src, dst_ref=dst, send_sem=ssem, recv_sem=rsem,
                                          device_id=dev(m), device_id_type=MESH_ID)
        cp.start()

    my_data = lax.axis_index("data")
    U[me] = jnp.concatenate([u0_ref[...], u1_ref[...], u2_ref[...], jnp.zeros((8 - n_layers, shard), F32)], axis=0)

    def cell(d, m):
        return {"data": d, "model": m}

    column = [(step, c) for step in range(1, n_data) for c in (core, 1 - core)]
    barrier = pltpu.get_barrier_semaphore()
    for step in range(1, n_model):
        pl.semaphore_signal(barrier, inc=1, device_id=dev((me + step) % n_model), device_id_type=MESH_ID)
    for step, c in column:
        pl.semaphore_signal(barrier, inc=1, device_id=cell((my_data + step) % n_data, chip * CORES + c),
                            device_id_type=MESH_ID)
    pl.semaphore_wait(barrier, n_model - 1 + len(column))

    mrow = pl.multiple_of(me * shard, shard)
    hs = shard // 2

    def send_w(k):
        for nb, rsem in ((right, wl), (left, wr)):
            remote(w_refs[k], W.at[k, pl.ds(mrow, shard)], w_send.at[k], rsem.at[k], nb * CORES + core)
        remote(w_refs[k], W.at[k, pl.ds(mrow, shard)], w_d2d.at[k], wp.at[k], partner)

    def rows_of(c):
        return pl.multiple_of((c * CORES + core) * shard, shard)

    def forward_w(k):
        src_l = W.at[k, pl.ds(rows_of(left), shard)]
        src_r = W.at[k, pl.ds(rows_of(right), shard)]
        wait_bytes(src_l, wl.at[k])
        half_l = W.at[k, pl.ds(rows_of(left), hs)]
        remote(half_l, half_l, w_fwd.at[k], wf.at[k], right * CORES + core)
        remote(src_l, src_l, w_d2d.at[k], wp.at[k], partner)
        wait_bytes(src_r, wr.at[k])
        half_r = W.at[k, pl.ds(rows_of(right) + hs, hs)]
        remote(half_r, half_r, w_fwd.at[k], wf.at[k], left * CORES + core)
        remote(src_r, src_r, w_d2d.at[k], wp.at[k], partner)

    def finish_w(k):
        src_f = W.at[k, pl.ds(rows_of(far), shard)]
        wait_bytes(src_f, wf.at[k])
        remote(src_f, src_f, w_d2d.at[k], wp.at[k], partner)
        wait_bytes(W.at[k, pl.ds(0, n_chips * shard)], wp.at[k])

    qrows = shard // n_data
    hrows = qrows // 2
    up = (my_data + 1) % n_data
    down = (my_data + n_data - 1) % n_data
    opp = (my_data + 2) % n_data
    to_up, to_down = {"data": up}, {"data": down}

    def w_part(k, c, d, off, n):
        return W.at[k, pl.ds(pl.multiple_of((c * CORES + core) * shard + d * qrows + off, hrows), n)]

    def remote_to(src, dst, ssem, rsem, device):
        pltpu.make_async_remote_copy(src_ref=src, dst_ref=dst, send_sem=ssem, recv_sem=rsem,
                                     device_id=device, device_id_type=MESH_ID).start()

    def send_wq(k):
        src = w_refs[k].at[pl.ds(pl.multiple_of(my_data * qrows, qrows), qrows)]
        for nb, rsem in ((right, wl), (left, wr), (far, wf)):
            remote(src, w_part(k, chip, my_data, 0, qrows), w_send.at[k], rsem.at[k], nb * CORES + core)
        remote(w_refs[k], W.at[k, pl.ds(mrow, shard)], w_d2d.at[k], wp.at[k], partner)

    def spread_wq(k):
        for c, rsem in ((left, wl), (right, wr), (far, wf)):
            ref = w_part(k, c, my_data, 0, qrows)
            wait_bytes(ref, rsem.at[k])
            remote_to(ref, ref, wy_send.at[k], wy_down.at[k], to_up)
            remote_to(ref, ref, wy_send.at[k], wy_up.at[k], to_down)

    def relay_wq(k):
        wait_bytes(W.at[k, pl.ds(0, 3 * qrows)], wy_down.at[k])
        for c in (left, right, far):
            ref = w_part(k, c, down, 0, hrows)
            remote_to(ref, ref, w_fwd.at[k], wy_far.at[k], to_up)
        wait_bytes(W.at[k, pl.ds(0, 3 * qrows)], wy_up.at[k])
        for c in (left, right, far):
            ref = w_part(k, c, up, hrows, hrows)
            remote_to(ref, ref, w_fwd.at[k], wy_far.at[k], to_down)

    def finish_wq(k):
        wait_bytes(W.at[k, pl.ds(0, 3 * qrows)], wy_far.at[k])
        for c in (left, right, far):
            ref = W.at[k, pl.ds(rows_of(c), shard)]
            remote(ref, ref, w_d2d.at[k], wp.at[k], partner)
        wait_bytes(W.at[k, pl.ds(0, n_chips * shard)], wp.at[k])

    def send_t(r):
        for c in range(CORES):
            src = t_hbm.at[pl.ds(c * rows + r * chunk, chunk)]
            dst = T.at[me, pl.ds(r * chunk, chunk)]
            for nb, rsem in ((right, tl), (left, tr)):
                remote(src, dst, t_send.at[r], rsem.at[r], nb * CORES + c)
        src = t_hbm.at[pl.ds(pl.multiple_of((1 - core) * rows + r * chunk, chunk), chunk)]
        remote(src, T.at[me, pl.ds(r * chunk, chunk)], t_send.at[r], tp.at[r], partner)

    def forward_t(r):
        wait_bytes(T.at[pl.ds(left * CORES, CORES), pl.ds(r * chunk, chunk)], tl.at[r])
        for c in range(CORES):
            ref = T.at[left * CORES + c, pl.ds(r * chunk, half)]
            remote(ref, ref, t_fwd.at[r], tf.at[r], right * CORES + core)
        wait_bytes(T.at[pl.ds(right * CORES, CORES), pl.ds(r * chunk, chunk)], tr.at[r])
        for c in range(CORES):
            ref = T.at[right * CORES + c, pl.ds(r * chunk + half, half)]
            remote(ref, ref, t_fwd.at[r], tf.at[r], left * CORES + core)

    def load_x(r, slot):
        return pltpu.make_async_copy(x_hbm.at[pl.ds(pl.multiple_of(row0 + r * chunk, chunk), chunk)],
                                     xb.at[slot], x_sem.at[slot])

    send_wq(1)
    send_wq(2)
    send_w(0)
    for step in range(1, n_model):
        remote(U.at[me], U.at[me], u_send, u_recv, (me + step) % n_model)
    send_t(0)
    own_t = pltpu.make_async_copy(t_hbm.at[pl.ds(pl.multiple_of(row0, rows), rows)], T.at[me], t_own)
    own_t.start()
    load_x(0, 0).start()
    load_x(1, 1).start()
    for k in range(n_layers):
        W[k, pl.ds(mrow, shard)] = w_refs[k][...]
    sums[...] = jnp.zeros_like(sums)
    dw_ref[...] = jnp.zeros_like(dw_ref)
    tiles[my_data * CORES + core] = jnp.zeros((8, LANES), F32)
    small_ref[...] = jnp.zeros_like(small_ref)
    spread_wq(1)
    spread_wq(2)
    wait_bytes(U.at[pl.ds(0, n_model - 1)], u_recv)
    wait_bytes(U.at[pl.ds(0, n_model - 1)], u_send)
    forward_w(0)
    send_t(1)
    relay_wq(1)
    for k in range(n_layers):
        if k == 0:
            finish_w(0)
        else:
            finish_wq(k)
        for i in range(width // NBLK):
            for j in range(width // NBLK):
                blk = W[k, i * NBLK:(i + 1) * NBLK, j * NBLK:(j + 1) * NBLK]
                WT[k, j * NBLK:(j + 1) * NBLK, i * NBLK:(i + 1) * NBLK] = blk.T
        u_all = jnp.concatenate([U[m] for m in range(n_model)], axis=1)
        p_all = dot(split3(u_all), W[k])
        p_row = p_all[k:k + 1] + p_all[8 + k:9 + k] + p_all[16 + k:17 + k]
        p_norm = jnp.sqrt(jnp.sum(p_row * p_row, axis=1, keepdims=True))
        v_row = p_row / jnp.maximum(p_norm, 1e-12)
        s_all = dot(split3(jnp.broadcast_to(v_row, (8, width))), WT[k])
        s_row = s_all[0:1] + s_all[8:9] + s_all[16:17]
        sigma = jnp.sqrt(jnp.sum(s_row * s_row, axis=1, keepdims=True))
        small_ref[k:k + 1] = v_row
        small_ref[n_layers + k:n_layers + k + 1] = s_row / sigma
        small_ref[2 * n_layers + k:2 * n_layers + k + 1] = jnp.broadcast_to(sigma, (1, width))
        if k == 0:
            relay_wq(2)
    for k in range(n_layers):
        wait_bytes(W.at[k, pl.ds(0, 3 * qrows if k else CORES * shard)], w_send.at[k])
        wait_bytes(W.at[k, pl.ds(0, 6 * hrows if k else shard)], w_fwd.at[k])
        if k:
            wait_bytes(W.at[k, pl.ds(0, 6 * qrows)], wy_send.at[k])
        wait_bytes(W.at[k, pl.ds(0, n_chips * shard)], w_d2d.at[k])
    own_t.wait()
    inv = [1.0 / small_ref[2 * n_layers + k:2 * n_layers + k + 1, 0:1] for k in range(n_layers)]
    blocks = [slice(n * NBLK, (n + 1) * NBLK) for n in range(width // NBLK)]
    own_cols = pl.multiple_of(chip * CORES * shard, CORES * shard)
    subs = [pl.ds(h * chunk, chunk) for h in range(2)]

    def fold(val):
        return jnp.sum(val.reshape(chunk // 8, 8, NBLK), axis=0)

    def body(i, carry):
        par = i % 2
        base = pl.multiple_of(2 * par, 2)
        for h in range(2):
            load_x(2 * i + h, base + h).wait()

        forward_t(2 * i)
        forward_t(2 * i + 1)

        @pl.when(2 * i + 2 < n_chunk)
        def _():
            for h in range(2):
                load_x(2 * i + 2 + h, 2 - base + h).start()
            send_t(2 * i + 2)
            send_t(2 * i + 3)

        xin = xb[pl.ds(base, 2)].reshape(2 * chunk, width)
        for blk in blocks:
            y_val = dot(xin, WT[0, :, blk]) * inv[0]
            y0[:, blk] = y_val
            x1[:, blk] = jnp.maximum(y_val, 0.2 * y_val).astype(BF16)
        for blk in blocks:
            y_val = dot(x1[...], WT[1, :, blk]) * inv[1]
            y1[:, blk] = y_val
            x2[:, blk] = jnp.maximum(y_val, 0.2 * y_val).astype(BF16)

        loss_sum = jnp.zeros((8, NBLK), F32)
        c_sum = [jnp.zeros((8, NBLK), F32) for _ in range(n_layers)]
        for h, sub in enumerate(subs):
            wait_bytes(T.at[pl.ds(far * CORES, CORES), pl.ds((2 * i + h) * chunk, chunk)], tf.at[2 * i + h])
            wait_bytes(T.at[partner, pl.ds((2 * i + h) * chunk, chunk)], tp.at[2 * i + h])
            trow = pl.ds(pl.multiple_of((2 * i + h) * chunk, chunk), chunk)
            for n, blk in enumerate(blocks):
                y_val = dot(x2[sub], WT[2, :, blk]) * inv[2]
                t_val = jnp.concatenate([T[2 * n, trow], T[2 * n + 1, trow]], axis=1).astype(F32)
                res = y_val - t_val
                loss_sum += fold(res * res)
                g_val = res * (1.0 / batch_total)
                c_sum[2] += fold(g_val * y_val)
                e2[sub, blk] = g_val.astype(BF16)

        def back(k, h, ek, yk, store):
            sub = subs[h]
            for blk in blocks:
                r_val = (dot(ek[sub], W[k, :, blk]) * inv[k]).astype(BF16).astype(F32)
                y_val = yk[sub, blk]
                g_val = jnp.where(y_val > 0, r_val, 0.2 * r_val)
                c_sum[k - 1] += fold(g_val * y_val)
                store(h, blk, g_val.astype(BF16))

        def store_e1(h, blk, val):
            e1[subs[h], blk] = val

        def store_e0(h, blk, val):
            e0[2 * i + h, :, blk] = val

        def weight_grad(k, e_own, x_val):
            dw_ref[k] += dot(e_own.T, x_val)

        back(2, 0, e2, y1, store_e1)
        back(2, 1, e2, y1, store_e1)
        weight_grad(2, e2[:, pl.ds(own_cols, CORES * shard)], x2[...])
        back(1, 0, e1, y0, store_e0)
        back(1, 1, e1, y0, store_e0)
        weight_grad(1, e1[:, pl.ds(own_cols, CORES * shard)], x1[...])
        for h in range(2):
            weight_grad(0, e0[2 * i + h, :, pl.ds(own_cols, CORES * shard)], xb[base + h])
        for k in range(n_layers):
            sums[k] += c_sum[k]
        sums[n_layers] += loss_sum
        return carry

    def out_rows(r):
        return pl.ds(pl.multiple_of(row0 + r * chunk, chunk), chunk)

    def out_copy(r, slot):
        return pltpu.make_async_copy(dxb.at[slot], dx_hbm.at[out_rows(r)], dx_loc.at[slot])

    def out_remote(r, slot):
        return pltpu.make_async_remote_copy(src_ref=dxb.at[slot], dst_ref=dx_hbm.at[out_rows(r)],
                                            send_sem=dx_send.at[slot], recv_sem=dx_recv.at[r],
                                            device_id=dev(partner), device_id_type=MESH_ID)

    def out_wait(r, slot):
        out_copy(r, slot).wait()
        out_remote(r, slot).wait_send()

    lax.fori_loop(0, n_chunk // 2, body, 0)

    pending = list(range(n_chunk))

    def next_dx():
        if not pending:
            return
        r = pending.pop(0)
        slot = r % 2
        if r >= 2:
            out_wait(r - 2, slot)
        for blk in blocks:
            dxb[slot, :, blk] = (dot(e0[r], W[0, :, blk]) * inv[0]).astype(BF16)
        out_copy(r, slot).start()
        out_remote(r, slot).start()


    for i in range(4):
        tot = jnp.sum(jnp.sum(sums[i], axis=0, keepdims=True), axis=1, keepdims=True)
        tiles[my_data * CORES + core, i:i + 1] = jnp.broadcast_to(tot, (1, LANES))
    mine = tiles.at[my_data * CORES + core]

    order = (2, 1, 0)
    mine_rows = pl.multiple_of(core * shard, shard)
    other_rows = pl.multiple_of((1 - core) * shard, shard)
    def quarter(d, off, n):
        return pl.ds(pl.multiple_of(d * qrows + off, 8), n)

    def acc_quarter(d, off, n):
        return pl.ds(pl.multiple_of(mine_rows + d * qrows + off, 8), n)

    for k in order:
        remote_to(dw_ref.at[k, pl.ds(other_rows, shard)], pair.at[k], p_send.at[k], p_recv.at[k], dev(partner))
    remote_to(mine, mine, s_send, s_recv, dev(partner))
    for step, c in column:
        remote_to(mine, mine, s_send, s_recv, cell((my_data + step) % n_data, chip * CORES + c))
    next_dx()
    for k in order:
        wait_bytes(pair.at[k], p_recv.at[k])
        dw_ref[k, pl.ds(mine_rows, shard)] += pair[k]
        remote_to(dw_ref.at[k, acc_quarter(opp, 0, hrows)], far_l.at[k], f_send.at[k], fl.at[k], to_up)
        remote_to(dw_ref.at[k, acc_quarter(opp, hrows, hrows)], far_r.at[k], f_send.at[k], fr.at[k], to_down)
        remote_to(dw_ref.at[k, acc_quarter(up, hrows, hrows)], near_l.at[k, pl.ds(hrows, hrows)], n_send.at[k], nl.at[k], to_up)
        remote_to(dw_ref.at[k, acc_quarter(down, 0, hrows)], near_r.at[k, pl.ds(0, hrows)], n_send.at[k], nr.at[k], to_down)
    next_dx()
    for k in order:
        next_dx()
        wait_bytes(far_l.at[k], fl.at[k])
        dw_ref[k, acc_quarter(up, 0, hrows)] += far_l[k]
        remote_to(dw_ref.at[k, acc_quarter(up, 0, hrows)], near_l.at[k, pl.ds(0, hrows)], n_send.at[k], nl.at[k], to_up)
        wait_bytes(far_r.at[k], fr.at[k])
        dw_ref[k, acc_quarter(down, hrows, hrows)] += far_r[k]
        remote_to(dw_ref.at[k, acc_quarter(down, hrows, hrows)], near_r.at[k, pl.ds(hrows, hrows)], n_send.at[k], nr.at[k], to_down)
    for k in order:
        next_dx()
        wait_bytes(near_l.at[k], nl.at[k])
        wait_bytes(near_r.at[k], nr.at[k])
        g_ref[k, quarter(my_data, 0, qrows)] = dw_ref[k, acc_quarter(my_data, 0, qrows)] + near_l[k] + near_r[k]
        ref = g_ref.at[k, quarter(my_data, 0, qrows)]
        remote_to(ref, ref, g_send.at[k], gl.at[k], to_up)
        remote_to(ref, ref, g_send.at[k], gr.at[k], to_down)
    for k in order:
        wait_bytes(g_ref.at[k, quarter(down, 0, qrows)], gl.at[k])
        ref = g_ref.at[k, quarter(down, 0, hrows)]
        remote_to(ref, ref, gf_send.at[k], gf.at[k], to_up)
        wait_bytes(g_ref.at[k, quarter(up, 0, qrows)], gr.at[k])
        ref = g_ref.at[k, quarter(up, hrows, hrows)]
        remote_to(ref, ref, gf_send.at[k], gf.at[k], to_down)

    while pending:
        next_dx()
    out_wait(n_chunk - 2, 0)
    out_wait(n_chunk - 1, 1)

    def drain(r, carry):
        wait_bytes(T.at[pl.ds(0, 2 * CORES + 1), pl.ds(0, chunk)], t_send.at[r])
        wait_bytes(T.at[pl.ds(0, CORES), pl.ds(0, chunk)], t_fwd.at[r])
        pltpu.make_async_copy(dxb.at[0], dxb.at[0], dx_recv.at[r]).wait()
        return carry

    lax.fori_loop(0, n_chunk, drain, 0)
    wait_bytes(tiles.at[pl.ds(0, len(column) + 1)], s_recv)
    wait_bytes(tiles.at[pl.ds(0, len(column) + 1)], s_send)
    total = tiles[0]
    for n in range(1, n_data * CORES):
        total = total + tiles[n]
    small_ref[9:13] = jnp.concatenate([total[0:4]] * (width // LANES), axis=1)
    for k in order:
        wait_bytes(g_ref.at[k, quarter(opp, 0, qrows)], gf.at[k])
        wait_bytes(pair.at[k], p_send.at[k])
        wait_bytes(near_l.at[k], f_send.at[k])
        wait_bytes(pair.at[k, pl.ds(0, 2 * qrows)], n_send.at[k])
        wait_bytes(pair.at[k, pl.ds(0, 2 * qrows)], g_send.at[k])
        wait_bytes(near_l.at[k], gf_send.at[k])


def finish_kernel(batch_total, dx_in, g_hbm, small_ref, dx_out, loss_ref, dw0, dw1, dw2,
                  un0, un1, un2, v0, v1, v2, sig_ref, buf, g_buf, d_buf, in_sem, out_sem, g_in, d_out):
    n_layers, shard, width = g_buf.shape
    slots, rows, _ = buf.shape
    me = lax.axis_index("model")
    loads = [pltpu.make_async_copy(dx_in.at[pl.ds(n * rows, rows)], buf.at[n], in_sem.at[n]) for n in range(slots)]
    stores = [pltpu.make_async_copy(buf.at[n], dx_out.at[pl.ds(n * rows, rows)], out_sem.at[n]) for n in range(slots)]
    g_load = pltpu.make_async_copy(g_hbm, g_buf, g_in)
    g_load.start()
    for load in loads:
        load.start()
    g_load.wait()
    mine = pl.ds(pl.multiple_of(me * shard, shard), shard)
    sigs, writes = [], []
    for k, (dw, un, v) in enumerate(((dw0, un0, v0), (dw1, un1, v1), (dw2, un2, v2))):
        v_row = small_ref[k:k + 1]
        u_row = small_ref[n_layers + k:n_layers + k + 1, mine]
        sigma = small_ref[2 * n_layers + k:2 * n_layers + k + 1, 0:1]
        scale = small_ref[3 * n_layers + k:3 * n_layers + k + 1, 0:1] / sigma
        u_col = jnp.broadcast_to(u_row, (8, shard)).T[:, 0:1]
        d_buf[k] = g_buf[k] * (1.0 / sigma) - (scale * u_col) * v_row
        writes.append(pltpu.make_async_copy(d_buf.at[k], dw, d_out.at[k]))
        un[...] = u_row
        v[...] = v_row
        sigs.append(sigma)
    sig_ref[...] = jnp.concatenate(sigs, axis=1)
    loss_ref[...] = (0.5 / batch_total) * small_ref[4 * n_layers:4 * n_layers + 1, 0:1]
    for write in writes:
        write.start()
    for load, store in zip(loads, stores):
        load.wait()
        store.start()
    for copy in stores + writes:
        copy.wait()


def solution(mesh):
    data_size = mesh.shape["data"]
    n_model = mesh.shape["model"]
    row_spec = P(("replica", "model"), None)
    vec_spec = P(("replica", "model"))
    batch_spec = P(("replica", "data"), None)
    target_spec = P(("replica", "data"), "model")
    part_spec = P("replica")

    def local_step(x_in, w_in, w_mid, w_out, u_in, u_mid, u_out, target):
        rows_all, width = x_in.shape
        shard = w_in.shape[0]
        batch_total = rows_all * data_size
        rows = rows_all // CORES
        chunk = rows // 8
        n_chunk = rows // chunk
        vm = pltpu.VMEM
        dma = pltpu.SemaphoreType.DMA
        any_spec = pl.BlockSpec(memory_space=pl.ANY)
        vmem_spec = pl.BlockSpec(memory_space=pltpu.VMEM)
        dx, g_mat, small = pl.pallas_call(
            functools.partial(stack_kernel, n_model, data_size, chunk, batch_total),
            out_shape=(jax.ShapeDtypeStruct((rows_all, width), BF16),
                       jax.ShapeDtypeStruct((3, shard, width), F32),
                       jax.ShapeDtypeStruct((16, width), F32)),
            in_specs=[vmem_spec] * 6 + [any_spec, any_spec],
            out_specs=(any_spec, vmem_spec, vmem_spec),
            scratch_shapes=[
                vm((3, CORES * shard, width), F32), vm((3, shard, width), F32),
                vm((3, shard // data_size // 2, width), F32), vm((3, shard // data_size // 2, width), F32),
                vm((3, shard // data_size, width), F32), vm((3, shard // data_size, width), F32),
                vm((data_size * CORES, 8, LANES), F32),
                vm((3, width, width), BF16), vm((3, width, width), BF16),
                vm((n_model, 8, shard), F32), vm((n_model, rows, shard), BF16),
                vm((4, chunk, width), BF16), vm((2 * chunk, width), BF16), vm((2 * chunk, width), BF16),
                vm((2 * chunk, width), F32), vm((2 * chunk, width), F32),
                vm((2 * chunk, width), BF16), vm((2 * chunk, width), BF16), vm((n_chunk, chunk, width), BF16),
                vm((2, chunk, width), BF16), vm((4, 8, NBLK), F32),
                dma, dma, *[dma((3,)) for _ in range(11)],
                dma, dma((n_chunk,)), dma((n_chunk,)), dma((n_chunk,)), dma((n_chunk,)), dma((n_chunk,)), dma((n_chunk,)),
                dma((4,)), dma((2,)), dma((2,)), dma((n_chunk,)),
                *[dma((3,)) for _ in range(13)], dma, dma],
            compiler_params=pltpu.CompilerParams(collective_id=0, has_side_effects=True,
                                                 vmem_limit_bytes=67043328),
        )(w_in, w_mid, w_out, u_in.reshape(1, shard), u_mid.reshape(1, shard), u_out.reshape(1, shard), x_in, target)

        slots = 32
        sds = jax.ShapeDtypeStruct
        outs = pl.pallas_call(
            functools.partial(finish_kernel, batch_total),
            out_shape=([sds((rows_all, width), BF16), sds((1, 1), F32)] + [sds((shard, width), F32)] * 3
                       + [sds((1, shard), F32)] * 3 + [sds((1, width), F32)] * 3 + [sds((1, 3), F32)]),
            in_specs=[any_spec, any_spec, vmem_spec],
            out_specs=[any_spec, vmem_spec] + [any_spec] * 3 + [vmem_spec] * 7,
            scratch_shapes=[vm((slots, rows_all // slots, width), BF16), vm((3, shard, width), F32), vm((3, shard, width), F32),
                            dma((slots,)), dma((slots,)), dma, dma((3,))],
        )(dx, g_mat, small)
        return (outs[1].reshape(1), outs[0], outs[2], outs[3], outs[4]) + tuple(o.reshape(-1) for o in outs[5:])

    in_specs = (batch_spec, row_spec, row_spec, row_spec, vec_spec, vec_spec, vec_spec, target_spec)
    out_specs = (part_spec, batch_spec, row_spec, row_spec, row_spec, vec_spec, vec_spec, vec_spec, part_spec, part_spec, part_spec, part_spec)
    return jax.shard_map(local_step, mesh=mesh, in_specs=in_specs, out_specs=out_specs, check_vma=False)
```
